32 devices in a mesh: dp: 8 (over z, x), heads: 4 (over y, core).
Axes of the slice: x: 2, y: 2, z: 4, core: 2. Of those that a mesh axis runs over, the one named last changes fastest.
Arguments:
- queries: bfloat16 [64, 16, 128], P('dp', 'heads'), may hold values from -12 to 12
- key_cache: bfloat16 [512, 8, 256, 128], P('dp', 'heads'), may hold values from -6 to 6
- value_cache: bfloat16 [512, 8, 256, 128], P('dp', 'heads'), may hold values from -6 to 6
- lengths_seen: int32 [64, 4], P('dp', 'heads'), may hold values from 1025 to 2048, as said below
- page_table: int32 [64, 8], P('dp'), may hold values from 0 to 63, as said below
- finished: int32 [64], P('dp'), may hold values from 0 to 1, as said below
- move_plan: int32 [256, 3], P('dp'), may hold values from 0 to 63, as said below
Outputs:
- attention: bfloat16 [64, 16, 128], P('dp', 'heads')
The draws below stay inside these ranges and needn't reach their ends.
Inputs may be any that keep to these rules, and one draw needn't show every extreme that they name: `lengths_seen`: each session's length, the largest entry of its row, lies between (5) * 256 + 1 and 2048. `page_table`: the 8 rows of one device's sessions hold each of that device's slot numbers exactly once. At most 2 sessions of one device are finished. `move_plan`: A row's source device differs from its receiving device; the destination slots of one receiving device are distinct, and each holds, after the moves, a page below the length of a session that is not finished. One device receives at most 5 pages from one source device, and on every device some source sends exactly 5.
All inputs are finite; a program needn't handle non-finite values.
Results may differ from the reference program's by a relative error of at most 0.008.
Values may be sent and summed in bfloat16 or wider, within the bound.
No kernel may reach another device: no remote copies, remote signals or barrier semaphores. Data moves between devices by JAX's collectives and lax.ppermute only.
A program may use at most 64 MiB of HBM per device.

```python
import jax
import jax.numpy as jnp
from jax import lax

HD = 128
QH = 16
KVH = 8
PAGE = 256
PAGES_MAX = 8
MOVES_DEV = 32
SESS_DEV = 8
SLOTS = 64
SESSIONS = 64
N_DP = 8
N_HEADS = 4


def joint_layout(key):
    base = jax.random.fold_in(key, 911)
    subkeys = jax.random.split(base, 9)
    device_ids = jnp.arange(N_DP, dtype=jnp.int32)
    true_length = jax.random.randint(subkeys[0], (N_DP, SESS_DEV), (PAGES_MAX - 3) * PAGE + 1, PAGES_MAX * PAGE + 1, dtype=jnp.int32)
    holder = jax.random.randint(subkeys[1], (N_DP, SESS_DEV, 1), 0, N_HEADS, dtype=jnp.int32)
    shortfall = jax.random.randint(subkeys[2], (N_DP, SESS_DEV, N_HEADS), 1, PAGE + 1, dtype=jnp.int32)
    columns = lax.broadcasted_iota(jnp.int32, (N_DP, SESS_DEV, N_HEADS), 2)
    seen = jnp.where(columns == holder, true_length[:, :, None], true_length[:, :, None] - shortfall)
    tables = jax.vmap(lambda sub: jax.random.permutation(sub, SLOTS))(jax.random.split(subkeys[3], N_DP)).astype(jnp.int32)
    order = jax.vmap(lambda sub: jax.random.permutation(sub, SESS_DEV))(jax.random.split(subkeys[4], N_DP)).astype(jnp.int32)
    coins = jax.random.randint(subkeys[5], (N_DP, SESS_DEV), 0, 2, dtype=jnp.int32)
    finished = jnp.where(order < SESS_DEV // 3, coins, 0).astype(jnp.int32)
    used_pages = (true_length + PAGE - 1) // PAGE
    page_index = lax.broadcasted_iota(jnp.int32, (N_DP, SESS_DEV, PAGES_MAX), 2)
    eligible = (page_index < used_pages[:, :, None]) & (finished[:, :, None] == 0)
    ranking = jax.vmap(lambda sub: jax.random.permutation(sub, SLOTS))(jax.random.split(subkeys[6], N_DP)).astype(jnp.int32)
    priority = eligible.reshape(N_DP, SLOTS).astype(jnp.int32) * SLOTS + ranking
    chosen = lax.top_k(priority, MOVES_DEV)[1].astype(jnp.int32)
    target = jnp.take_along_axis(tables, chosen, axis=1)
    offsets = jax.vmap(lambda sub: jax.random.permutation(sub, N_DP - 1))(jax.random.split(subkeys[7], N_DP)).astype(jnp.int32) + 1
    rows = jnp.arange(MOVES_DEV, dtype=jnp.int32)
    offset_index = rows % (N_DP - 1)
    source_device = (device_ids[:, None] + offsets[:, offset_index]) % N_DP
    source_slot = jax.random.randint(subkeys[8], (N_DP, MOVES_DEV), 0, SLOTS, dtype=jnp.int32)
    plan = jnp.stack([source_device, source_slot, target], axis=2).reshape(N_DP * MOVES_DEV, 3).astype(jnp.int32)
    return (seen.reshape(SESSIONS, N_HEADS), tables.reshape(SESSIONS, PAGES_MAX), finished.reshape(SESSIONS), plan)


def draw_lengths_seen(key, part):
    return joint_layout(key)[0]


def draw_page_table(key, part):
    return joint_layout(key)[1]


def draw_finished(key, part):
    return joint_layout(key)[2]


def draw_move_plan(key, part):
    return joint_layout(key)[3]


def shard_levels(own_key, extent, cuts, least, high):
    def one(position, parts):
        draws = jax.random.uniform(jax.random.fold_in(jax.random.fold_in(own_key, 6), position), (parts,), jnp.float32, least / len(cuts), high / len(cuts))
        return jnp.repeat(jnp.exp(draws), extent[position] // parts).reshape((-1,) + (1,) * (len(extent) - position - 1))

    factor_of = one(*cuts[0])
    for cut in cuts[1:]:
        factor_of = factor_of * one(*cut)
    return factor_of


def normal_values(rng, extent, deviation, most, cuts=(), kind=jnp.bfloat16):
    gain = shard_levels(rng, extent, cuts, -0.22, 0.18) if cuts else 1.0
    result = jax.random.normal(rng, extent, jnp.float32) * deviation * gain
    return jnp.minimum(jnp.maximum(result, -most), most).astype(kind)


def setup_inputs(seed: int = 0) -> dict:
    streams_of = jax.random.split(jax.random.key(seed), 8)
    queries = normal_values(streams_of[0], (SESSIONS, QH, HD), 2.0, 12.0, ((0, 8), (1, 4)))
    key_cache = normal_values(streams_of[1], (N_DP * SLOTS, KVH, PAGE, HD), 1.0, 6.0, ((0, 8), (1, 4)))
    value_cache = normal_values(streams_of[2], (N_DP * SLOTS, KVH, PAGE, HD), 1.0, 6.0, ((0, 8), (1, 4)))
    lengths_seen = draw_lengths_seen(jax.random.fold_in(streams_of[7], 71), 0)
    page_table = draw_page_table(jax.random.fold_in(streams_of[7], 71), 0)
    finished = draw_finished(jax.random.fold_in(streams_of[7], 71), 0)
    move_plan = draw_move_plan(jax.random.fold_in(streams_of[7], 71), 0)
    return dict(queries=queries, key_cache=key_cache, value_cache=value_cache, lengths_seen=lengths_seen, page_table=page_table, finished=finished, move_plan=move_plan)


softcap_limit = 50.0
score_divisor = 12.0


def reference(queries, key_cache, value_cache, lengths_seen, page_table, finished, move_plan):
    key_pages = key_cache.reshape(N_DP, SLOTS, KVH, PAGE, HD)
    value_pages = value_cache.reshape(N_DP, SLOTS, KVH, PAGE, HD)
    receiver = (jnp.arange(N_DP * MOVES_DEV, dtype=jnp.int32) // MOVES_DEV).astype(jnp.int32)
    source_device = move_plan[:, 0]
    source_slot = move_plan[:, 1]
    target_slot = move_plan[:, 2]
    key_pages = key_pages.at[receiver, target_slot].set(key_pages[source_device, source_slot])
    value_pages = value_pages.at[receiver, target_slot].set(value_pages[source_device, source_slot])
    length = jnp.max(lengths_seen, axis=1)
    home = (jnp.arange(SESSIONS, dtype=jnp.int32) // SESS_DEV).astype(jnp.int32)
    group_size = QH // KVH

    def attend_session(inputs):
        query_row, slot_row, device, session_length, is_finished = inputs
        picked_keys = key_pages[device, slot_row]
        picked_values = value_pages[device, slot_row]
        token_keys = picked_keys.transpose(1, 0, 2, 3).reshape(KVH, PAGES_MAX * PAGE, HD).astype(jnp.float32)
        token_values = picked_values.transpose(1, 0, 2, 3).reshape(KVH, PAGES_MAX * PAGE, HD).astype(jnp.float32)
        grouped = query_row.reshape(KVH, group_size, HD).astype(jnp.float32)
        raw_scores = jnp.einsum('kgd,ktd->kgt', grouped, token_keys, precision=lax.Precision.HIGHEST) / score_divisor
        capped = softcap_limit * jnp.tanh(raw_scores / softcap_limit)
        places = lax.broadcasted_iota(jnp.int32, capped.shape, 2)
        weights = jnp.where(places < session_length, jnp.exp(capped), jnp.float32(0.0)).astype(jnp.bfloat16)
        weights = lax.optimization_barrier(weights).astype(jnp.float32)
        numerator = jnp.einsum('kgt,ktd->kgd', weights, token_values, precision=lax.Precision.HIGHEST)
        denominator = jnp.sum(weights, axis=2)
        output = (numerator / denominator[:, :, None]).reshape(QH, HD)
        return jnp.where(is_finished == 1, jnp.float32(0.0), output).astype(jnp.bfloat16)

    return lax.map(attend_session, (queries, page_table, home, length, finished))
```

```python
import functools
import math

import jax
import jax.numpy as jnp
from jax import lax
from jax.experimental import pallas as pl
from jax.experimental.pallas import tpu as pltpu
from jax.sharding import PartitionSpec as P

softcap_limit = 50.0
score_divisor = 12.0
exp_scale = softcap_limit * math.log2(math.e)
BATCH = 4
LEN_BASE = 128
SESS_LANE, PAGE_LANE, HIGH_LANE, LOW_LANE = 32, 64, 96, 112

VMEM = pl.BlockSpec(memory_space=pltpu.VMEM)
SMEM = pl.BlockSpec(memory_space=pltpu.SMEM)
HBM = pl.BlockSpec(memory_space=pl.ANY)


def pack_kernel(n_heads, len_ref, table_ref, plan_ref, query_ref, out_ref, owner, count, meta):
    sessions, pages_max = table_ref.shape
    moves = plan_ref.shape[0]
    devices, tiles = out_ref.shape[:2]
    n_dp = devices // n_heads
    rows = out_ref.shape[2]
    lane = lax.broadcasted_iota(jnp.int32, (1, 128), 1)
    base = jnp.zeros((1, 128), jnp.int32)
    for s in range(sessions):
        length = len_ref[s, 0]
        base = jnp.where(lane == HIGH_LANE + s, length // LEN_BASE, base)
        base = jnp.where(lane == LOW_LANE + s, length % LEN_BASE, base)
        for p in range(pages_max):
            owner[table_ref[s, p]] = s * pages_max + p
    for d in range(n_dp):
        count[d] = 0
        meta[d] = base
    for r in range(moves):
        source = plan_ref[r, 0]
        rank = count[source]
        count[source] = rank + 1
        entry = owner[plan_ref[r, 2]]
        session = entry // pages_max
        page = entry % pages_max
        row = meta[source]
        row = jnp.where(lane == rank, plan_ref[r, 1] + 1, row)
        row = jnp.where(lane == SESS_LANE + rank, session, row)
        row = jnp.where(lane == PAGE_LANE + rank, page, row)
        meta[source] = row
        tile = query_ref[session]
        for h in range(n_heads):
            out_ref[source * n_heads + h, rank] = tile
    for d in range(n_dp):
        row = jnp.broadcast_to(meta[d].astype(jnp.float32), (rows, 128)).astype(jnp.bfloat16)
        for h in range(n_heads):
            out_ref[d * n_heads + h, tiles - 1] = row


def decode_lengths(block):
    return block * LEN_BASE + pltpu.roll(block, 128 - (LOW_LANE - HIGH_LANE), block.ndim - 1)


def page_sums(kv_heads, page_size, query, key_of, value_of, live):
    rows = query.shape[0]
    group = rows // kv_heads
    row = lax.broadcasted_iota(jnp.int32, (rows, page_size), 0)
    raw = None
    for k in range(kv_heads):
        part = lax.dot_general(
            query, key_of(k), (((1,), (1,)), ((), ())), preferred_element_type=jnp.float32
        )
        raw = part if raw is None else jnp.where(row < k * group, raw, part)
    capped = jnp.tanh(raw * (1.0 / (score_divisor * softcap_limit)))
    place = lax.broadcasted_iota(jnp.int32, (rows, page_size), 1)
    weight = jnp.where(place < live, jnp.exp2(capped * exp_scale), 0.0).astype(jnp.bfloat16)
    total = jnp.sum(weight.astype(jnp.float32), axis=1, keepdims=True)
    out = None
    out_row = lax.broadcasted_iota(jnp.int32, (rows, 128), 0)
    for k in range(kv_heads):
        part = jnp.dot(weight, value_of(k), preferred_element_type=jnp.float32)
        out = part if out is None else jnp.where(out_row < k * group, out, part)
    return out, total


def run_pages(entries, total, get_query, key_hbm, value_hbm, key_buf, value_buf, sems, num, den):
    kv_heads, page_size = key_hbm.shape[1:3]
    batches = (total + BATCH - 1) // BATCH

    def pad(i, carry):
        entries[0, i] = 0
        entries[1, i] = 0
        entries[2, i] = 0
        return carry

    lax.fori_loop(total, batches * BATCH, pad, 0)

    def start(i, carry):
        slot = entries[0, i]
        pltpu.make_async_copy(key_hbm.at[slot], key_buf.at[i], sems.at[0, i]).start()
        pltpu.make_async_copy(value_hbm.at[slot], value_buf.at[i], sems.at[1, i]).start()
        return carry

    lax.fori_loop(0, batches * BATCH, start, 0)

    def batch(b, carry):
        first = b * BATCH
        for j in range(BATCH):
            i = first + j
            pltpu.make_async_copy(key_hbm.at[0], key_buf.at[i], sems.at[0, i]).wait()
            pltpu.make_async_copy(value_hbm.at[0], value_buf.at[i], sems.at[1, i]).wait()
        results = []
        for j in range(BATCH):
            i = first + j
            results.append(
                page_sums(
                    kv_heads,
                    page_size,
                    get_query(i),
                    lambda k, i=i: key_buf[i, k],
                    lambda k, i=i: value_buf[i, k],
                    entries[1, i],
                )
            )
        for j in range(BATCH):
            row = entries[2, first + j]
            out, total_weight = results[j]
            num[row] = num[row] + out
            den[row] = den[row] + jnp.broadcast_to(total_weight, out.shape)
        return carry

    lax.fori_loop(0, batches, batch, 0)


def remote_kernel(
    n_heads, recv_ref, key_hbm, value_hbm, out_ref,
    meta, scalars, copied, entries, origin, key_buf, value_buf, sems, num, den,
):
    devices, tiles, rows = recv_ref.shape[:3]
    n_dp = devices // n_heads
    capacity = tiles - 1
    sessions = out_ref.shape[1] - 1
    page_size = key_hbm.shape[2]
    head = lax.axis_index("heads")
    lane = lax.broadcasted_iota(jnp.int32, (1, 128), 1)
    for d in range(n_dp):
        own = recv_ref[d * n_heads + head, capacity].astype(jnp.float32).astype(jnp.int32)[0:1]
        longest = None
        for h in range(n_heads):
            block = recv_ref[d * n_heads + h, capacity].astype(jnp.float32).astype(jnp.int32)[0:1]
            length = decode_lengths(block)
            longest = length if longest is None else jnp.maximum(longest, length)
        meta[d : d + 1, :] = jnp.where(lane >= HIGH_LANE, longest, own)
    copy = pltpu.make_async_copy(meta, scalars, copied)
    copy.start()
    num[...] = jnp.zeros_like(num)
    den[...] = jnp.zeros_like(den)
    copy.wait()

    total = jnp.int32(0)
    for d in range(n_dp):
        for c in range(capacity):
            slot = scalars[d, c]
            session = scalars[d, SESS_LANE + c]
            page = scalars[d, PAGE_LANE + c]
            live = jnp.clip(scalars[d, HIGH_LANE + session] - page * page_size, 0, page_size)

            @pl.when(slot > 0)
            def _(slot=slot, live=live, session=session, total=total, d=d, c=c):
                entries[0, total] = slot - 1
                entries[1, total] = live
                entries[2, total] = d * sessions + session
                origin[total] = d * capacity + c

            total = total + (slot > 0).astype(jnp.int32)

    def query(i):
        place = origin[i]
        return recv_ref[(place // capacity) * n_heads + head, place % capacity]

    def clear(i, carry):
        origin[i] = 0
        return carry

    lax.fori_loop(total, (total + BATCH - 1) // BATCH * BATCH, clear, 0)
    run_pages(entries, total, query, key_hbm, value_hbm, key_buf, value_buf, sems, num, den)

    tile_lane = lax.broadcasted_iota(jnp.int32, (rows, 128), 1)
    for d in range(n_dp):
        packed = jnp.zeros((rows, 128), jnp.float32)
        for s in range(sessions):
            out_ref[d, s] = num[d * sessions + s].astype(jnp.bfloat16)
            value = den[d * sessions + s]
            high = value.astype(jnp.bfloat16).astype(jnp.float32)
            packed = jnp.where(tile_lane == s, high, packed)
            packed = jnp.where(tile_lane == 64 + s, value - high, packed)
        out_ref[d, sessions] = packed.astype(jnp.bfloat16)


def local_kernel(
    n_heads, recv_ref, table_ref, plan_ref, finished_ref, query_ref, key_hbm, value_hbm,
    num, den, meta, scalars, copied, entries, moved, key_buf, value_buf, sems,
):
    capacity = recv_ref.shape[1] - 1
    sessions, pages_max = table_ref.shape
    page_size = key_hbm.shape[2]
    slots = key_hbm.shape[0]
    d = lax.axis_index("dp")
    longest = None
    for h in range(n_heads):
        block = recv_ref[d * n_heads + h, capacity].astype(jnp.float32).astype(jnp.int32)[0:1]
        length = decode_lengths(block)
        longest = length if longest is None else jnp.maximum(longest, length)
    meta[...] = jnp.broadcast_to(longest, meta.shape)
    copy = pltpu.make_async_copy(meta, scalars, copied)
    copy.start()
    num[...] = jnp.zeros_like(num)
    den[...] = jnp.zeros_like(den)
    for j in range(slots):
        moved[j] = 0
    for r in range(plan_ref.shape[0]):
        moved[plan_ref[r, 2]] = 1
    copy.wait()
    total = jnp.int32(0)
    for s in range(sessions):
        length = jnp.where(finished_ref[s] == 1, 0, scalars[0, HIGH_LANE + s])
        for p in range(pages_max):
            slot = table_ref[s, p]
            live = jnp.clip(length - p * page_size, 0, page_size)
            needed = (live > 0) & (moved[slot] == 0)

            @pl.when(needed)
            def _(slot=slot, live=live, total=total, s=s):
                entries[0, total] = slot
                entries[1, total] = live
                entries[2, total] = s

            total = total + needed.astype(jnp.int32)

    def query(i):
        return query_ref[entries[2, i]]

    run_pages(entries, total, query, key_hbm, value_hbm, key_buf, value_buf, sems, num, den)


def combine_kernel(finished_ref, back_ref, num_ref, den_ref, out_ref):
    n_dp, tiles, rows = back_ref.shape[:3]
    sessions = tiles - 1
    packed = back_ref[0, sessions].astype(jnp.float32)
    for d in range(1, n_dp):
        packed = packed + back_ref[d, sessions].astype(jnp.float32)
    packed = packed + pltpu.roll(packed, 64, 1)
    for s in range(sessions):
        total = num_ref[s]
        for d in range(n_dp):
            total = total + back_ref[d, s].astype(jnp.float32)
        weight = den_ref[s] + jnp.broadcast_to(packed[:, s : s + 1], (rows, 128))
        done = finished_ref[s] == 1
        out_ref[s] = jnp.where(done, 0.0, total / jnp.where(done, 1.0, weight)).astype(jnp.bfloat16)


def body(queries, key_cache, value_cache, lengths_seen, page_table, finished, move_plan):
    slot_total, kv_heads, page_size, head_dim = key_cache.shape
    sessions, q_heads, _ = queries.shape
    pages_max = page_table.shape[1]
    moves = move_plan.shape[0]
    n_dp = lax.axis_size("dp")
    n_heads = lax.axis_size("heads")
    capacity = (moves - 1) // (n_dp - 1) + 1
    assert capacity <= 32 and sessions <= 16 and slot_total < 256 and pages_max <= 256
    asked_max = -(-n_dp * capacity // BATCH) * BATCH
    local_max = -(-sessions * pages_max // BATCH) * BATCH

    packed = pl.pallas_call(
        functools.partial(pack_kernel, n_heads),
        out_shape=jax.ShapeDtypeStruct(
            (n_dp * n_heads, capacity + 1, q_heads, head_dim), jnp.bfloat16
        ),
        in_specs=[SMEM, SMEM, SMEM, VMEM],
        out_specs=VMEM,
        scratch_shapes=[
            pltpu.SMEM((slot_total,), jnp.int32),
            pltpu.SMEM((n_dp,), jnp.int32),
            pltpu.VMEM((n_dp, 1, 128), jnp.int32),
        ],
        name="pack",
    )(lengths_seen, page_table, move_plan, queries)
    recv = lax.all_to_all(packed, ("dp", "heads"), split_axis=0, concat_axis=0, tiled=True)

    def page_scratch(count):
        return [
            pltpu.VMEM((count, kv_heads, page_size, head_dim), jnp.bfloat16),
            pltpu.VMEM((count, kv_heads, page_size, head_dim), jnp.bfloat16),
            pltpu.SemaphoreType.DMA((2, count)),
        ]

    response = pl.pallas_call(
        functools.partial(remote_kernel, n_heads),
        out_shape=jax.ShapeDtypeStruct((n_dp, sessions + 1, q_heads, head_dim), jnp.bfloat16),
        in_specs=[VMEM, HBM, HBM],
        out_specs=VMEM,
        scratch_shapes=[
            pltpu.VMEM((n_dp, 128), jnp.int32),
            pltpu.SMEM((n_dp, 128), jnp.int32),
            pltpu.SemaphoreType.DMA,
            pltpu.SMEM((3, asked_max), jnp.int32),
            pltpu.SMEM((asked_max,), jnp.int32),
            *page_scratch(asked_max),
            pltpu.VMEM((n_dp * sessions, q_heads, head_dim), jnp.float32),
            pltpu.VMEM((n_dp * sessions, q_heads, head_dim), jnp.float32),
        ],
        name="remote_pages",
        cost_estimate=pl.CostEstimate(flops=10**8, transcendentals=0, bytes_accessed=10**7),
    )(recv, key_cache, value_cache)
    back = lax.all_to_all(response, "dp", split_axis=0, concat_axis=0, tiled=True)
    accumulator = jax.ShapeDtypeStruct((sessions, q_heads, head_dim), jnp.float32)
    num, den = pl.pallas_call(
        functools.partial(local_kernel, n_heads),
        out_shape=(accumulator, accumulator),
        in_specs=[VMEM, SMEM, SMEM, SMEM, VMEM, HBM, HBM],
        out_specs=(VMEM, VMEM),
        scratch_shapes=[
            pltpu.VMEM((8, 128), jnp.int32),
            pltpu.SMEM((8, 128), jnp.int32),
            pltpu.SemaphoreType.DMA,
            pltpu.SMEM((3, local_max), jnp.int32),
            pltpu.SMEM((slot_total,), jnp.int32),
            *page_scratch(local_max),
        ],
        name="local_pages",
        cost_estimate=pl.CostEstimate(flops=10**9, transcendentals=0, bytes_accessed=10**7),
    )(recv, page_table, move_plan, finished, queries, key_cache, value_cache)
    return pl.pallas_call(
        combine_kernel,
        out_shape=jax.ShapeDtypeStruct((sessions, q_heads, head_dim), jnp.bfloat16),
        in_specs=[SMEM, VMEM, VMEM, VMEM],
        out_specs=VMEM,
        name="combine",
    )(finished, back, num, den)


def solution(mesh):
    in_specs = (
        P("dp", "heads", None),
        P("dp", "heads", None, None),
        P("dp", "heads", None, None),
        P("dp", "heads"),
        P("dp", None),
        P("dp"),
        P("dp", None),
    )
    out_specs = P("dp", "heads", None)
    return jax.shard_map(body, mesh=mesh, in_specs=in_specs, out_specs=out_specs, check_vma=False)
```

```python
import functools
import math

import jax
import jax.numpy as jnp
from jax import lax
from jax.experimental import pallas as pl
from jax.experimental.pallas import tpu as pltpu
from jax.sharding import PartitionSpec as P

softcap_limit = 50.0
score_divisor = 12.0
exp_scale = softcap_limit * math.log2(math.e)
GROUP = 4
LEN_BASE = 128
SMALL_VMEM = 4 << 20
SESS_LANE, PAGE_LANE, HIGH_LANE, LOW_LANE = 32, 64, 96, 112

VMEM = pl.BlockSpec(memory_space=pltpu.VMEM)
HBM = pl.BlockSpec(memory_space=pltpu.HBM)


def in_hbm(array):
    return pltpu.with_memory_space_constraint(array, pltpu.HBM)


def load_all(pairs, sems):
    copies = [pltpu.make_async_copy(s, d, sems.at[i]) for i, (s, d) in enumerate(pairs)]
    for copy in copies:
        copy.start()
    return copies


def pack_kernel(
    n_heads, len_hbm, table_hbm, plan_hbm, query_hbm, out_ref,
    len_ref, table_ref, plan_ref, query_ref, sems, owner, count, meta,
):
    copies = load_all(
        [(len_hbm, len_ref), (table_hbm, table_ref), (plan_hbm, plan_ref), (query_hbm, query_ref)],
        sems,
    )
    sessions, pages_max = table_ref.shape
    moves = plan_ref.shape[1]
    devices, tiles = out_ref.shape[:2]
    n_dp = devices // n_heads
    rows = out_ref.shape[2]
    head = lax.axis_index("heads")
    lane = lax.broadcasted_iota(jnp.int32, (1, 128), 1)
    base = jnp.zeros((1, 128), jnp.int32)
    for d in range(n_dp):
        count[d] = 0
    for copy in copies:
        copy.wait()
    for s in range(sessions):
        length = len_ref[0, s]
        base = jnp.where(lane == HIGH_LANE + s, length // LEN_BASE, base)
        base = jnp.where(lane == LOW_LANE + s, length % LEN_BASE, base)
        for p in range(pages_max):
            owner[table_ref[s, p]] = s * 256 + p
    for d in range(n_dp):
        meta[d] = base
    for r in range(moves):
        source = plan_ref[0, r]
        rank = count[source]
        count[source] = rank + 1
        entry = owner[plan_ref[2, r]]
        session = entry >> 8
        row = meta[source]
        row = jnp.where(lane == rank, plan_ref[1, r] + 1, row)
        row = jnp.where(lane == SESS_LANE + rank, session, row)
        row = jnp.where(lane == PAGE_LANE + rank, entry & 255, row)
        meta[source] = row
        out_ref[source * n_heads + head, rank] = query_ref[session]
    for d in range(n_dp):
        row = jnp.broadcast_to(meta[d].astype(jnp.float32), (rows, 128)).astype(jnp.bfloat16)
        for h in range(n_heads):
            out_ref[d * n_heads + h, tiles - 1] = row


def decode(recv_ref, index):
    tile = recv_ref[index, recv_ref.shape[1] - 1]
    return tile.astype(jnp.float32).astype(jnp.int32)[0:1]


def longest_of(recv_ref, d, n_heads):
    longest = None
    for h in range(n_heads):
        block = decode(recv_ref, d * n_heads + h)
        length = block * LEN_BASE + pltpu.roll(block, 128 - (LOW_LANE - HIGH_LANE), 1)
        longest = length if longest is None else jnp.maximum(longest, length)
    return longest


class Pages:
    def __init__(self, key_hbm, value_hbm, entries, key_buf, value_buf, sems, num, den):
        self.key_hbm, self.value_hbm, self.entries = key_hbm, value_hbm, entries
        self.key_buf, self.value_buf, self.sems = key_buf, value_buf, sems
        self.num, self.den = num, den
        self.kv_heads, self.page_size = key_hbm.shape[1:3]
        self.rows = num.shape[1]
        self.group = self.rows // self.kv_heads

    def start(self, i, slot):
        pltpu.make_async_copy(
            self.key_hbm.at[slot], self.key_buf.at[i], self.sems.at[0, i]
        ).start()
        pltpu.make_async_copy(
            self.value_hbm.at[slot], self.value_buf.at[i], self.sems.at[1, i]
        ).start()

    def add(self, total, needed, slot, live, row, query):
        @pl.when(needed)
        def _():
            self.start(total, slot)
            self.entries[0, total] = total
            self.entries[1, total] = live
            self.entries[2, total] = row
            self.entries[3, total] = query

        return total + needed.astype(jnp.int32)

    def wait(self, first, total, which):
        buf, hbm = (self.key_buf, self.key_hbm) if which == 0 else (self.value_buf, self.value_hbm)
        for j in range(GROUP):
            i = first + j

            @pl.when(i < total)
            def _(i=i):
                pltpu.make_async_copy(hbm.at[0], buf.at[i], self.sems.at[which, i]).wait()

    def scores(self, first, get_query):
        raws = []
        for j in range(GROUP):
            i = first + j
            query = get_query(self.entries[3, i])
            buffer = self.entries[0, i]
            raws.append(
                [
                    lax.dot_general(
                        query,
                        self.key_buf[buffer, k],
                        (((1,), (1,)), ((), ())),
                        preferred_element_type=jnp.float32,
                    )
                    for k in range(self.kv_heads)
                ]
            )
        return raws

    def select(self, parts):
        row = lax.broadcasted_iota(jnp.int32, parts[0].shape, 0)
        out = parts[-1]
        for k in reversed(range(self.kv_heads - 1)):
            out = jnp.where(row < (k + 1) * self.group, parts[k], out)
        return out

    def weights(self, first, raws):
        out = []
        place = lax.broadcasted_iota(jnp.int32, (self.rows, self.page_size), 1)
        for j in range(GROUP):
            raw = self.select(raws[j])
            capped = jnp.tanh(raw * (1.0 / (score_divisor * softcap_limit)))
            weight = jnp.exp2(capped * exp_scale)
            live = self.entries[1, first + j]
            out.append(jnp.where(place < live, weight, 0.0).astype(jnp.bfloat16))
        return out

    def products(self, first, weights):
        parts = []
        for j in range(GROUP):
            buffer = self.entries[0, first + j]
            parts.append(
                [
                    jnp.dot(
                        weights[j], self.value_buf[buffer, k], preferred_element_type=jnp.float32
                    )
                    for k in range(self.kv_heads)
                ]
            )
        return parts

    def accumulate(self, first, weights, parts):
        for j in range(GROUP):
            row = self.entries[2, first + j]
            total = jnp.sum(weights[j].astype(jnp.float32), axis=1, keepdims=True)
            out = self.select(parts[j])
            self.num[row] = self.num[row] + out
            self.den[row] = self.den[row] + jnp.broadcast_to(total, out.shape)

    def run(self, total, get_query):
        for j in range(GROUP):
            for field in range(4):
                self.entries[field, total + j] = 0

        @pl.when(total == 0)
        def _():
            self.start(0, 0)

        total = jnp.maximum(total, 1)
        groups = (total + GROUP - 1) // GROUP
        self.wait(0, total, 0)
        weights = self.weights(0, self.scores(0, get_query))

        def step(g, weights):
            first = g * GROUP
            before = first - GROUP
            self.wait(first, total, 0)
            self.wait(before, total, 1)
            raws = self.scores(first, get_query)
            parts = self.products(before, weights)
            later = self.weights(first, raws)
            self.accumulate(before, weights, parts)
            return later

        weights = lax.fori_loop(1, groups, step, weights)
        last = (groups - 1) * GROUP
        self.wait(last, total, 1)
        self.accumulate(last, weights, self.products(last, weights))


def remote_kernel(
    n_heads, recv_ref, key_hbm, value_hbm, out_ref,
    meta, scalars, copied, num, den, entries, key_buf, value_buf, sems,
):
    devices, tiles, rows = recv_ref.shape[:3]
    n_dp = devices // n_heads
    capacity = tiles - 1
    sessions = out_ref.shape[1] - 1
    page_size = key_hbm.shape[2]
    head = lax.axis_index("heads")
    lane = lax.broadcasted_iota(jnp.int32, (1, 128), 1)
    for d in range(n_dp):
        own = decode(recv_ref, d * n_heads + head)
        meta[d : d + 1, :] = jnp.where(
            lane >= HIGH_LANE, longest_of(recv_ref, d, n_heads), own
        )
    copy = pltpu.make_async_copy(meta, scalars, copied)
    copy.start()
    num[...] = jnp.zeros_like(num)
    den[...] = jnp.zeros_like(den)
    queries_ref = recv_ref.reshape(devices * tiles, rows, recv_ref.shape[3])
    copy.wait()

    pages = Pages(key_hbm, value_hbm, entries, key_buf, value_buf, sems, num, den)
    total = jnp.int32(0)
    for d in range(n_dp):
        for c in range(capacity):
            slot = scalars[d, c]
            session = scalars[d, SESS_LANE + c]
            page = scalars[d, PAGE_LANE + c]
            live = jnp.clip(scalars[d, HIGH_LANE + session] - page * page_size, 0, page_size)
            total = pages.add(
                total,
                slot > 0,
                slot - 1,
                live,
                d * sessions + session,
                (d * n_heads + head) * tiles + c,
            )
    pages.run(total, lambda tile: queries_ref[tile])

    tile_lane = lax.broadcasted_iota(jnp.int32, (rows, 128), 1)
    for d in range(n_dp):
        packed = jnp.zeros((rows, 128), jnp.float32)
        for s in range(sessions):
            out_ref[d, s] = num[d * sessions + s].astype(jnp.bfloat16)
            value = den[d * sessions + s]
            high = value.astype(jnp.bfloat16).astype(jnp.float32)
            packed = jnp.where(tile_lane == s, high, packed)
            packed = jnp.where(tile_lane == 64 + s, value - high, packed)
        out_ref[d, sessions] = packed.astype(jnp.bfloat16)


def local_kernel(
    n_heads, recv_ref, table_hbm, plan_hbm, finished_hbm, query_hbm, key_hbm, value_hbm,
    num, den, table_ref, plan_ref, finished_ref, query_ref, loads, meta, scalars, copied,
    moved, entries, key_buf, value_buf, sems,
):
    copies = load_all(
        [
            (table_hbm, table_ref),
            (plan_hbm, plan_ref),
            (finished_hbm, finished_ref),
            (query_hbm, query_ref),
        ],
        loads,
    )
    sessions, pages_max = table_ref.shape
    page_size = key_hbm.shape[2]
    slots = key_hbm.shape[0]
    longest = longest_of(recv_ref, lax.axis_index("dp"), n_heads)
    meta[...] = jnp.broadcast_to(longest, meta.shape)
    copy = pltpu.make_async_copy(meta, scalars, copied)
    copy.start()
    num[...] = jnp.zeros_like(num)
    for j in range(slots):
        moved[j] = 0
    for load in copies:
        load.wait()
    for s in range(sessions):
        den[s] = jnp.full(den.shape[1:], 1.0, jnp.float32) * finished_ref[0, s].astype(jnp.float32)
    for r in range(plan_ref.shape[1]):
        moved[plan_ref[2, r]] = 1
    copy.wait()
    pages = Pages(key_hbm, value_hbm, entries, key_buf, value_buf, sems, num, den)
    total = jnp.int32(0)
    for s in range(sessions):
        length = jnp.where(finished_ref[0, s] == 1, 0, scalars[0, HIGH_LANE + s])
        for p in range(pages_max):
            slot = table_ref[s, p]
            live = jnp.clip(length - p * page_size, 0, page_size)
            needed = (live > 0) & (moved[slot] == 0)
            total = pages.add(total, needed, slot, live, s, s)
    pages.run(total, lambda session: query_ref[session])


def combine_kernel(back_ref, num_ref, den_ref, out_ref):
    n_dp, tiles, rows = back_ref.shape[:3]
    sessions = tiles - 1
    packed = back_ref[0, sessions].astype(jnp.float32)
    for d in range(1, n_dp):
        packed = packed + back_ref[d, sessions].astype(jnp.float32)
    packed = packed + pltpu.roll(packed, 64, 1)
    for s in range(sessions):
        total = num_ref[s]
        for d in range(n_dp):
            total = total + back_ref[d, s].astype(jnp.float32)
        weight = den_ref[s] + jnp.broadcast_to(packed[:, s : s + 1], (rows, 128))
        out_ref[s] = (total / weight).astype(jnp.bfloat16)


def body(queries, key_cache, value_cache, lengths_seen, page_table, finished, move_plan):
    slot_total, kv_heads, page_size, head_dim = key_cache.shape
    sessions, q_heads, _ = queries.shape
    pages_max = page_table.shape[1]
    moves = move_plan.shape[0]
    n_dp = lax.axis_size("dp")
    n_heads = lax.axis_size("heads")
    capacity = (moves - 1) // (n_dp - 1) + 1
    assert capacity <= 32 and sessions <= 16 and slot_total < 256 and pages_max <= 256

    seen = in_hbm(lengths_seen.T)
    plan = in_hbm(move_plan.T)
    table = in_hbm(page_table)
    query = in_hbm(queries)
    done = in_hbm(finished.reshape(1, sessions))
    keys = in_hbm(key_cache)
    values = in_hbm(value_cache)

    packed = pl.pallas_call(
        functools.partial(pack_kernel, n_heads),
        out_shape=jax.ShapeDtypeStruct(
            (n_dp * n_heads, capacity + 1, q_heads, head_dim), jnp.bfloat16
        ),
        in_specs=[HBM] * 4,
        out_specs=VMEM,
        scratch_shapes=[
            pltpu.SMEM((1, sessions), jnp.int32),
            pltpu.SMEM((sessions, pages_max), jnp.int32),
            pltpu.SMEM(plan.shape, jnp.int32),
            pltpu.VMEM(queries.shape, queries.dtype),
            pltpu.SemaphoreType.DMA((4,)),
            pltpu.SMEM((slot_total,), jnp.int32),
            pltpu.SMEM((n_dp,), jnp.int32),
            pltpu.VMEM((n_dp, 1, 128), jnp.int32),
        ],
        compiler_params=pltpu.CompilerParams(vmem_limit_bytes=SMALL_VMEM),
        name="pack",
    )(seen, table, plan, query)
    recv = lax.all_to_all(packed, ("dp", "heads"), split_axis=0, concat_axis=0, tiled=True)

    def page_scratch(count):
        buffer = pltpu.VMEM((count, kv_heads, page_size, head_dim), jnp.bfloat16)
        return [
            pltpu.SMEM((4, count + GROUP), jnp.int32),
            buffer,
            buffer,
            pltpu.SemaphoreType.DMA((2, count)),
        ]

    def page_limit(count):
        pages = 2 * count * kv_heads * page_size * head_dim * 2
        return pltpu.CompilerParams(vmem_limit_bytes=pages + SMALL_VMEM)

    asked = n_dp * capacity
    response = pl.pallas_call(
        functools.partial(remote_kernel, n_heads),
        out_shape=jax.ShapeDtypeStruct((n_dp, sessions + 1, q_heads, head_dim), jnp.bfloat16),
        in_specs=[VMEM, HBM, HBM],
        out_specs=VMEM,
        scratch_shapes=[
            pltpu.VMEM((n_dp, 128), jnp.int32),
            pltpu.SMEM((n_dp, 128), jnp.int32),
            pltpu.SemaphoreType.DMA,
            pltpu.VMEM((n_dp * sessions, q_heads, head_dim), jnp.float32),
            pltpu.VMEM((n_dp * sessions, q_heads, head_dim), jnp.float32),
            *page_scratch(asked),
        ],
        compiler_params=page_limit(asked),
        name="remote_pages",
        cost_estimate=pl.CostEstimate(flops=10**8, transcendentals=0, bytes_accessed=10**7),
    )(recv, keys, values)
    back = lax.all_to_all(response, "dp", split_axis=0, concat_axis=0, tiled=True)
    held = sessions * pages_max
    accumulator = jax.ShapeDtypeStruct((sessions, q_heads, head_dim), jnp.float32)
    num, den = pl.pallas_call(
        functools.partial(local_kernel, n_heads),
        out_shape=(accumulator, accumulator),
        in_specs=[VMEM, HBM, HBM, HBM, HBM, HBM, HBM],
        out_specs=(VMEM, VMEM),
        scratch_shapes=[
            pltpu.SMEM((sessions, pages_max), jnp.int32),
            pltpu.SMEM(plan.shape, jnp.int32),
            pltpu.SMEM((1, sessions), jnp.int32),
            pltpu.VMEM(queries.shape, queries.dtype),
            pltpu.SemaphoreType.DMA((4,)),
            pltpu.VMEM((8, 128), jnp.int32),
            pltpu.SMEM((8, 128), jnp.int32),
            pltpu.SemaphoreType.DMA,
            pltpu.SMEM((slot_total,), jnp.int32),
            *page_scratch(held),
        ],
        compiler_params=page_limit(held),
        name="local_pages",
        cost_estimate=pl.CostEstimate(flops=10**9, transcendentals=0, bytes_accessed=10**7),
    )(recv, table, plan, done, query, keys, values)
    return pl.pallas_call(
        combine_kernel,
        out_shape=jax.ShapeDtypeStruct((sessions, q_heads, head_dim), jnp.bfloat16),
        in_specs=[VMEM, VMEM, VMEM],
        out_specs=VMEM,
        compiler_params=pltpu.CompilerParams(vmem_limit_bytes=SMALL_VMEM),
        name="combine",
    )(back, num, den)


def solution(mesh):
    in_specs = (
        P("dp", "heads", None),
        P("dp", "heads", None, None),
        P("dp", "heads", None, None),
        P("dp", "heads"),
        P("dp", None),
        P("dp"),
        P("dp", None),
    )
    out_specs = P("dp", "heads", None)
    return jax.shard_map(body, mesh=mesh, in_specs=in_specs, out_specs=out_specs, check_vma=False)
```

```python
import functools
import math

import jax
import jax.numpy as jnp
from jax import lax
from jax.experimental import pallas as pl
from jax.experimental.pallas import tpu as pltpu
from jax.sharding import PartitionSpec as P

softcap_limit = 50.0
score_divisor = 12.0
exp_scale = softcap_limit * math.log2(math.e)
GROUP = 5
LEN_BASE = 128
SMALL_VMEM = 4 << 20
SESS_LANE, PAGE_LANE, HIGH_LANE, LOW_LANE = 32, 64, 96, 112

VMEM = pl.BlockSpec(memory_space=pltpu.VMEM)
HBM = pl.BlockSpec(memory_space=pltpu.HBM)


def in_hbm(array):
    return pltpu.with_memory_space_constraint(array, pltpu.HBM)


def load_all(pairs, sems):
    copies = [pltpu.make_async_copy(s, d, sems.at[i]) for i, (s, d) in enumerate(pairs)]
    for copy in copies:
        copy.start()
    return copies


def pack_kernel(
    n_heads, len_hbm, table_hbm, plan_hbm, query_hbm, out_ref,
    len_ref, table_ref, plan_ref, query_ref, sems, owner, count, meta,
):
    copies = load_all(
        [(len_hbm, len_ref), (table_hbm, table_ref), (plan_hbm, plan_ref), (query_hbm, query_ref)],
        sems,
    )
    sessions, pages_max = table_ref.shape
    moves = plan_ref.shape[1]
    devices, tiles = out_ref.shape[:2]
    n_dp = devices // n_heads
    rows = out_ref.shape[2]
    head = lax.axis_index("heads")
    lane = lax.broadcasted_iota(jnp.int32, (1, 128), 1)
    base = jnp.zeros((1, 128), jnp.int32)
    for d in range(n_dp):
        count[d] = 0
    for copy in copies:
        copy.wait()
    for s in range(sessions):
        length = len_ref[0, s]
        base = jnp.where(lane == HIGH_LANE + s, length // LEN_BASE, base)
        base = jnp.where(lane == LOW_LANE + s, length % LEN_BASE, base)
        for p in range(pages_max):
            owner[table_ref[s, p]] = s * 256 + p
    for d in range(n_dp):
        meta[d] = base
    for r in range(moves):
        source = plan_ref[0, r]
        rank = count[source]
        count[source] = rank + 1
        entry = owner[plan_ref[2, r]]
        session = entry >> 8
        row = meta[source]
        row = jnp.where(lane == rank, plan_ref[1, r] + 1, row)
        row = jnp.where(lane == SESS_LANE + rank, session, row)
        row = jnp.where(lane == PAGE_LANE + rank, entry & 255, row)
        meta[source] = row
        out_ref[source * n_heads + head, rank] = query_ref[session]
    for d in range(n_dp):
        row = jnp.broadcast_to(meta[d].astype(jnp.float32), (rows, 128)).astype(jnp.bfloat16)
        for h in range(n_heads):
            out_ref[d * n_heads + h, tiles - 1] = row


def decode(recv_ref, index):
    tile = recv_ref[index, recv_ref.shape[1] - 1]
    return tile.astype(jnp.float32).astype(jnp.int32)[0:1]


def longest_of(recv_ref, d, n_heads):
    longest = None
    for h in range(n_heads):
        block = decode(recv_ref, d * n_heads + h)
        length = block * LEN_BASE + pltpu.roll(block, 128 - (LOW_LANE - HIGH_LANE), 1)
        longest = length if longest is None else jnp.maximum(longest, length)
    return longest


class Pages:
    def __init__(self, key_hbm, value_hbm, words, key_buf, value_buf, sems, num, den):
        self.key_hbm, self.value_hbm, self.words = key_hbm, value_hbm, words
        self.key_buf, self.value_buf, self.sems = key_buf, value_buf, sems
        self.num, self.den = num, den
        self.kv_heads, self.page_size = key_hbm.shape[1:3]
        self.rows = num.shape[1]
        self.group = self.rows // self.kv_heads
        self.live_shift = key_hbm.shape[0].bit_length()
        self.row_shift = self.live_shift + self.page_size.bit_length()

    def word(self, slot, live, row):
        return (slot + 1) + live * (1 << self.live_shift) + row * (1 << self.row_shift)

    def slot(self, word):
        return (word & ((1 << self.live_shift) - 1)) - 1

    def live(self, i):
        return (self.words[i] >> self.live_shift) & (2 * self.page_size - 1)

    def row(self, i):
        return self.words[i] >> self.row_shift

    def buffer(self, i):
        return jnp.minimum(i, self.total - 1)

    def start(self, i, slot, which):
        buf, hbm = (self.key_buf, self.key_hbm) if which == 0 else (self.value_buf, self.value_hbm)
        pltpu.make_async_copy(hbm.at[slot], buf.at[i], self.sems.at[which, i]).start()

    def add(self, total, needed, word):
        @pl.when(needed)
        def _():
            self.start(total, self.slot(word), 0)
            self.words[total] = word

        @pl.when(needed & (total >= GROUP))
        def _():
            before = total - GROUP
            self.start(before, self.slot(self.words[before]), 1)

        return total + needed.astype(jnp.int32)

    def wait(self, first, which):
        buf, hbm = (self.key_buf, self.key_hbm) if which == 0 else (self.value_buf, self.value_hbm)
        for j in range(GROUP):
            i = first + j

            @pl.when(i < self.total)
            def _(i=i):
                pltpu.make_async_copy(hbm.at[0], buf.at[i], self.sems.at[which, i]).wait()

    def scores(self, first, get_query):
        raws = []
        for j in range(GROUP):
            i = first + j
            query = get_query(i)
            buffer = self.buffer(i)
            raws.append(
                [
                    lax.dot_general(
                        query,
                        self.key_buf[buffer, k],
                        (((1,), (1,)), ((), ())),
                        preferred_element_type=jnp.float32,
                    )
                    for k in range(self.kv_heads)
                ]
            )
        return raws

    def select(self, parts):
        row = lax.broadcasted_iota(jnp.int32, parts[0].shape, 0)
        out = parts[-1]
        for k in reversed(range(self.kv_heads - 1)):
            out = jnp.where(row < (k + 1) * self.group, parts[k], out)
        return out

    def weights(self, first, raws):
        out = []
        place = lax.broadcasted_iota(jnp.int32, (self.rows, self.page_size), 1)
        for j in range(GROUP):
            raw = self.select(raws[j])
            capped = jnp.tanh(raw * (1.0 / (score_divisor * softcap_limit)))
            weight = jnp.exp2(capped * exp_scale)
            live = self.live(first + j)
            out.append(jnp.where(place < live, weight, 0.0).astype(jnp.bfloat16))
        return out

    def products(self, first, weights):
        parts = []
        for j in range(GROUP):
            buffer = self.buffer(first + j)
            parts.append(
                [
                    jnp.dot(
                        weights[j], self.value_buf[buffer, k], preferred_element_type=jnp.float32
                    )
                    for k in range(self.kv_heads)
                ]
            )
        return parts

    def accumulate(self, first, weights, parts):
        for j in range(GROUP):
            row = self.row(first + j)
            total = jnp.sum(weights[j].astype(jnp.float32), axis=1, keepdims=True)
            out = self.select(parts[j])
            self.num[row] = self.num[row] + out
            self.den[row] = self.den[row] + jnp.broadcast_to(total, out.shape)

    def run(self, total, get_query):
        for j in range(GROUP):
            self.words[total + j] = 0

        @pl.when(total == 0)
        def _():
            self.start(0, 0, 0)
            self.words[0] = self.word(0, 0, 0)

        total = jnp.maximum(total, 1)
        self.total = total

        def rest(i, carry):
            self.start(i, self.slot(self.words[i]), 1)
            return carry

        lax.fori_loop(jnp.maximum(total - GROUP, 0), total, rest, 0)
        groups = (total + GROUP - 1) // GROUP
        self.wait(0, 0)
        weights = self.weights(0, self.scores(0, get_query))

        def step(g, weights):
            first = g * GROUP
            before = first - GROUP
            self.wait(first, 0)
            self.wait(before, 1)
            raws = self.scores(first, get_query)
            parts = self.products(before, weights)
            later = self.weights(first, raws)
            self.accumulate(before, weights, parts)
            return later

        weights = lax.fori_loop(1, groups, step, weights)
        last = (groups - 1) * GROUP
        self.wait(last, 1)
        self.accumulate(last, weights, self.products(last, weights))


def remote_kernel(
    n_heads, recv_ref, key_hbm, value_hbm, out_ref,
    meta, num, den, tiles_of, words, key_buf, value_buf, sems,
):
    devices, tiles, rows = recv_ref.shape[:3]
    n_dp = devices // n_heads
    capacity = tiles - 1
    sessions = out_ref.shape[1] - 1
    page_size = key_hbm.shape[2]
    head = lax.axis_index("heads")
    for d in range(n_dp):
        meta[0, d : d + 1, :] = decode(recv_ref, d * n_heads + head)
        meta[1, d : d + 1, :] = longest_of(recv_ref, d, n_heads)
    own, longest = meta[0], meta[1]
    session = pltpu.roll(own, 128 - SESS_LANE, 1)
    page = pltpu.roll(own, 128 - PAGE_LANE, 1)
    length = jnp.zeros_like(own)
    for s in range(sessions):
        known = jnp.broadcast_to(longest[:, HIGH_LANE + s : HIGH_LANE + s + 1], own.shape)
        length = jnp.where(session == s, known, length)
    live = jnp.clip(length - page * page_size, 0, page_size)
    pages = Pages(key_hbm, value_hbm, words, key_buf, value_buf, sems, num, den)
    device = lax.broadcasted_iota(jnp.int32, own.shape, 0)
    asked = jnp.where(own > 0, pages.word(own - 1, live, device * sessions + session), 0)
    num[...] = jnp.zeros_like(num)
    den[...] = jnp.zeros_like(den)
    queries_ref = recv_ref.reshape(devices * tiles, rows, recv_ref.shape[3])

    total = jnp.int32(0)
    for d in range(n_dp):
        for c in range(capacity):
            word = asked[d, c]
            tiles_of[total] = (d * n_heads + head) * tiles + c
            total = pages.add(total, word > 0, word)
    for j in range(GROUP):
        tiles_of[total + j] = 0
    pages.run(total, lambda i: queries_ref[tiles_of[i]])

    tile_lane = lax.broadcasted_iota(jnp.int32, (rows, 128), 1)
    for d in range(n_dp):
        packed = jnp.zeros((rows, 128), jnp.float32)
        for s in range(sessions):
            out_ref[d, s] = num[d * sessions + s].astype(jnp.bfloat16)
            value = den[d * sessions + s]
            high = value.astype(jnp.bfloat16).astype(jnp.float32)
            packed = jnp.where(tile_lane == s, high, packed)
            packed = jnp.where(tile_lane == 64 + s, value - high, packed)
        out_ref[d, sessions] = packed.astype(jnp.bfloat16)


def local_kernel(
    n_heads, recv_ref, table_hbm, plan_hbm, finished_hbm, query_hbm, key_hbm, value_hbm,
    num, den, table_ref, plan_ref, finished_ref, query_ref, loads,
    moved, words, key_buf, value_buf, sems,
):
    copies = load_all(
        [
            (table_hbm, table_ref),
            (plan_hbm, plan_ref),
            (finished_hbm, finished_ref),
            (query_hbm, query_ref),
        ],
        loads,
    )
    sessions, pages_max = table_ref.shape
    page_size = key_hbm.shape[2]
    slots = key_hbm.shape[0]
    longest = longest_of(recv_ref, lax.axis_index("dp"), n_heads)
    num[...] = jnp.zeros_like(num)
    for j in range(slots):
        moved[j] = 0
    for load in copies:
        load.wait()
    for s in range(sessions):
        den[s] = jnp.full(den.shape[1:], 1.0, jnp.float32) * finished_ref[0, s].astype(jnp.float32)
    for r in range(plan_ref.shape[1]):
        moved[plan_ref[2, r]] = 1
    pages = Pages(key_hbm, value_hbm, words, key_buf, value_buf, sems, num, den)
    total = jnp.int32(0)
    for s in range(sessions):
        length = jnp.where(finished_ref[0, s] == 1, 0, longest[0, HIGH_LANE + s])
        for p in range(pages_max):
            slot = table_ref[s, p]
            live = jnp.clip(length - p * page_size, 0, page_size)
            needed = (live > 0) & (moved[slot] == 0)
            total = pages.add(total, needed, pages.word(slot, live, s))
    pages.run(total, lambda i: query_ref[pages.row(i)])


def combine_kernel(back_ref, num_ref, den_ref, out_ref):
    n_dp, tiles, rows = back_ref.shape[:3]
    sessions = tiles - 1
    packed = back_ref[0, sessions].astype(jnp.float32)
    for d in range(1, n_dp):
        packed = packed + back_ref[d, sessions].astype(jnp.float32)
    packed = packed + pltpu.roll(packed, 64, 1)
    for s in range(sessions):
        total = num_ref[s]
        for d in range(n_dp):
            total = total + back_ref[d, s].astype(jnp.float32)
        weight = den_ref[s] + jnp.broadcast_to(packed[:, s : s + 1], (rows, 128))
        out_ref[s] = (total / weight).astype(jnp.bfloat16)


def body(queries, key_cache, value_cache, lengths_seen, page_table, finished, move_plan):
    slot_total, kv_heads, page_size, head_dim = key_cache.shape
    sessions, q_heads, _ = queries.shape
    pages_max = page_table.shape[1]
    moves = move_plan.shape[0]
    n_dp = lax.axis_size("dp")
    n_heads = lax.axis_size("heads")
    capacity = (moves - 1) // (n_dp - 1) + 1
    assert capacity <= 32 and sessions <= 16 and slot_total < 256 and pages_max <= 256
    assert page_size & (page_size - 1) == 0 and n_dp * sessions << 8 << 10 < 2**31

    seen = in_hbm(lengths_seen.T)
    plan = in_hbm(move_plan.T)
    table = in_hbm(page_table)
    query = in_hbm(queries)
    done = in_hbm(finished.reshape(1, sessions))
    keys = in_hbm(key_cache)
    values = in_hbm(value_cache)

    packed = pl.pallas_call(
        functools.partial(pack_kernel, n_heads),
        out_shape=jax.ShapeDtypeStruct(
            (n_dp * n_heads, capacity + 1, q_heads, head_dim), jnp.bfloat16
        ),
        in_specs=[HBM] * 4,
        out_specs=VMEM,
        scratch_shapes=[
            pltpu.SMEM((1, sessions), jnp.int32),
            pltpu.SMEM((sessions, pages_max), jnp.int32),
            pltpu.SMEM(plan.shape, jnp.int32),
            pltpu.VMEM(queries.shape, queries.dtype),
            pltpu.SemaphoreType.DMA((4,)),
            pltpu.SMEM((slot_total,), jnp.int32),
            pltpu.SMEM((n_dp,), jnp.int32),
            pltpu.VMEM((n_dp, 1, 128), jnp.int32),
        ],
        compiler_params=pltpu.CompilerParams(vmem_limit_bytes=SMALL_VMEM),
        name="pack",
    )(seen, table, plan, query)
    recv = lax.all_to_all(packed, ("dp", "heads"), split_axis=0, concat_axis=0, tiled=True)

    def page_scratch(count):
        buffer = pltpu.VMEM((count, kv_heads, page_size, head_dim), jnp.bfloat16)
        return [
            pltpu.SMEM((count + GROUP,), jnp.int32),
            buffer,
            buffer,
            pltpu.SemaphoreType.DMA((2, count)),
        ]

    def page_limit(count):
        pages = 2 * count * kv_heads * page_size * head_dim * 2
        return pltpu.CompilerParams(vmem_limit_bytes=pages + SMALL_VMEM)

    asked = n_dp * capacity
    response = pl.pallas_call(
        functools.partial(remote_kernel, n_heads),
        out_shape=jax.ShapeDtypeStruct((n_dp, sessions + 1, q_heads, head_dim), jnp.bfloat16),
        in_specs=[VMEM, HBM, HBM],
        out_specs=VMEM,
        scratch_shapes=[
            pltpu.VMEM((2, n_dp, 128), jnp.int32),
            pltpu.VMEM((n_dp * sessions, q_heads, head_dim), jnp.float32),
            pltpu.VMEM((n_dp * sessions, q_heads, head_dim), jnp.float32),
            pltpu.SMEM((asked + GROUP,), jnp.int32),
            *page_scratch(asked),
        ],
        compiler_params=page_limit(asked),
        name="remote_pages",
        cost_estimate=pl.CostEstimate(flops=10**8, transcendentals=0, bytes_accessed=10**7),
    )(recv, keys, values)
    back = lax.all_to_all(response, "dp", split_axis=0, concat_axis=0, tiled=True)
    held = sessions * pages_max
    accumulator = jax.ShapeDtypeStruct((sessions, q_heads, head_dim), jnp.float32)
    num, den = pl.pallas_call(
        functools.partial(local_kernel, n_heads),
        out_shape=(accumulator, accumulator),
        in_specs=[VMEM, HBM, HBM, HBM, HBM, HBM, HBM],
        out_specs=(VMEM, VMEM),
        scratch_shapes=[
            pltpu.SMEM((sessions, pages_max), jnp.int32),
            pltpu.SMEM(plan.shape, jnp.int32),
            pltpu.SMEM((1, sessions), jnp.int32),
            pltpu.VMEM(queries.shape, queries.dtype),
            pltpu.SemaphoreType.DMA((4,)),
            pltpu.SMEM((slot_total,), jnp.int32),
            *page_scratch(held),
        ],
        compiler_params=page_limit(held),
        name="local_pages",
        cost_estimate=pl.CostEstimate(flops=10**9, transcendentals=0, bytes_accessed=10**7),
    )(recv, table, plan, done, query, keys, values)
    return pl.pallas_call(
        combine_kernel,
        out_shape=jax.ShapeDtypeStruct((sessions, q_heads, head_dim), jnp.bfloat16),
        in_specs=[VMEM, VMEM, VMEM],
        out_specs=VMEM,
        compiler_params=pltpu.CompilerParams(vmem_limit_bytes=SMALL_VMEM),
        name="combine",
    )(back, num, den)


def solution(mesh):
    in_specs = (
        P("dp", "heads", None),
        P("dp", "heads", None, None),
        P("dp", "heads", None, None),
        P("dp", "heads"),
        P("dp", None),
        P("dp"),
        P("dp", None),
    )
    out_specs = P("dp", "heads", None)
    return jax.shard_map(body, mesh=mesh, in_specs=in_specs, out_specs=out_specs, check_vma=False)
```

```python
import functools
import math

import jax
import jax.numpy as jnp
from jax import lax
from jax.experimental import pallas as pl
from jax.experimental.pallas import tpu as pltpu
from jax.sharding import PartitionSpec as P

softcap_limit = 50.0
score_divisor = 12.0
exp_scale = softcap_limit * math.log2(math.e)
GROUP = 5
LEN_BASE = 128
SMALL_VMEM = 4 << 20
SESS_LANE, PAGE_LANE, HIGH_LANE, LOW_LANE = 32, 64, 96, 112

VMEM = pl.BlockSpec(memory_space=pltpu.VMEM)
HBM = pl.BlockSpec(memory_space=pltpu.HBM)


def in_hbm(array):
    return pltpu.with_memory_space_constraint(array, pltpu.HBM)


def load_all(pairs, sems):
    copies = [pltpu.make_async_copy(s, d, sems.at[i]) for i, (s, d) in enumerate(pairs)]
    for copy in copies:
        copy.start()
    return copies


def pack_kernel(
    n_heads, len_hbm, table_hbm, plan_hbm, query_hbm, out_ref,
    len_ref, table_ref, plan_ref, query_ref, sems, owner, count, meta,
):
    copies = load_all(
        [(len_hbm, len_ref), (table_hbm, table_ref), (plan_hbm, plan_ref), (query_hbm, query_ref)],
        sems,
    )
    sessions, pages_max = table_ref.shape
    moves = plan_ref.shape[1]
    devices, tiles = out_ref.shape[:2]
    n_dp = devices // n_heads
    rows = out_ref.shape[2]
    parts = query_ref.shape[1] // rows
    head = lax.axis_index("heads")
    lane = lax.broadcasted_iota(jnp.int32, (1, 128), 1)
    base = jnp.zeros((1, 128), jnp.int32)
    for d in range(n_dp):
        count[d] = 0
    for copy in copies:
        copy.wait()
    for s in range(sessions):
        length = len_ref[0, s]
        base = jnp.where(lane == HIGH_LANE + s, length // LEN_BASE, base)
        base = jnp.where(lane == LOW_LANE + s, length % LEN_BASE, base)
        for p in range(pages_max):
            owner[table_ref[s, p]] = s * 256 + p
    for d in range(n_dp):
        meta[d] = base
    for r in range(moves):
        source = plan_ref[0, r]
        rank = count[source]
        count[source] = rank + 1
        entry = owner[plan_ref[2, r]]
        session = entry >> 8
        row = meta[source]
        row = jnp.where(lane == rank, plan_ref[1, r] + 1, row)
        row = jnp.where(lane == SESS_LANE + rank, session, row)
        row = jnp.where(lane == PAGE_LANE + rank, entry & 255, row)
        meta[source] = row
        tile = query_ref[session]
        for k in range(parts):
            out_ref[source * n_heads + head, rank * parts + k] = tile[k * rows : (k + 1) * rows]
    for d in range(n_dp):
        row = jnp.broadcast_to(meta[d].astype(jnp.float32), (rows, 128)).astype(jnp.bfloat16)
        for h in range(n_heads):
            out_ref[d * n_heads + h, tiles - 1] = row


def decode(recv_ref, index):
    tile = recv_ref[index, recv_ref.shape[1] - 1]
    return tile.astype(jnp.float32).astype(jnp.int32)[0:1]


def longest_of(recv_ref, d, n_heads):
    longest = None
    for h in range(n_heads):
        block = decode(recv_ref, d * n_heads + h)
        length = block * LEN_BASE + pltpu.roll(block, 128 - (LOW_LANE - HIGH_LANE), 1)
        longest = length if longest is None else jnp.maximum(longest, length)
    return longest


class Pages:
    def __init__(
        self, key_hbm, value_hbm, words, key_buf, value_buf, sems, num, den, per_device=None
    ):
        self.key_hbm, self.value_hbm, self.words = key_hbm, value_hbm, words
        self.key_buf, self.value_buf, self.sems = key_buf, value_buf, sems
        self.num, self.den, self.per_device = num, den, per_device
        self.kv_heads, self.page_size = key_hbm.shape[1:3]
        self.rows = num.shape[1]
        self.group = self.rows // self.kv_heads
        self.live_shift = key_hbm.shape[0].bit_length()
        self.row_shift = self.live_shift + self.page_size.bit_length()

    def word(self, slot, live, row):
        return (slot + 1) + live * (1 << self.live_shift) + row * (1 << self.row_shift)

    def slot(self, word):
        return (word & ((1 << self.live_shift) - 1)) - 1

    def live(self, i):
        return (self.words[i] >> self.live_shift) & (2 * self.page_size - 1)

    def row(self, i):
        return self.words[i] >> self.row_shift

    def buffer(self, i):
        return jnp.minimum(i, self.total - 1)

    def start(self, i, slot, which):
        buf, hbm = (self.key_buf, self.key_hbm) if which == 0 else (self.value_buf, self.value_hbm)
        pltpu.make_async_copy(hbm.at[slot], buf.at[i], self.sems.at[which, i]).start()

    def add(self, total, needed, word):
        @pl.when(needed)
        def _():
            self.start(total, self.slot(word), 0)
            self.words[total] = word

        @pl.when(needed & (total >= GROUP))
        def _():
            before = total - GROUP
            self.start(before, self.slot(self.words[before]), 1)

        return total + needed.astype(jnp.int32)

    def wait(self, first, which):
        buf, hbm = (self.key_buf, self.key_hbm) if which == 0 else (self.value_buf, self.value_hbm)
        for j in range(GROUP):
            i = first + j

            @pl.when(i < self.total)
            def _(i=i):
                pltpu.make_async_copy(hbm.at[0], buf.at[i], self.sems.at[which, i]).wait()

    def scores(self, first, get_query):
        raws = []
        for j in range(GROUP):
            i = first + j
            query = get_query(i)
            buffer = self.buffer(i)
            raws.append(
                [
                    lax.dot_general(
                        query,
                        self.key_buf[buffer, k],
                        (((1,), (1,)), ((), ())),
                        preferred_element_type=jnp.float32,
                    )
                    for k in range(self.kv_heads)
                ]
            )
        return raws

    def select(self, parts):
        row = lax.broadcasted_iota(jnp.int32, parts[0].shape, 0)
        out = parts[-1]
        for k in reversed(range(self.kv_heads - 1)):
            out = jnp.where(row < (k + 1) * self.group, parts[k], out)
        return out

    def weights(self, first, raws):
        out = []
        place = lax.broadcasted_iota(jnp.int32, (self.rows, self.page_size), 1)
        for j in range(GROUP):
            raw = self.select(raws[j])
            capped = jnp.tanh(raw * (1.0 / (score_divisor * softcap_limit)))
            weight = jnp.exp2(capped * exp_scale)
            live = self.live(first + j)
            out.append(jnp.where(place < live, weight, 0.0).astype(jnp.bfloat16))
        return out

    def products(self, first, weights):
        parts = []
        for j in range(GROUP):
            buffer = self.buffer(first + j)
            parts.append(
                [
                    jnp.dot(
                        weights[j], self.value_buf[buffer, k], preferred_element_type=jnp.float32
                    )
                    for k in range(self.kv_heads)
                ]
            )
        return parts

    def accumulate(self, first, weights, parts):
        for j in range(GROUP):
            row = self.row(first + j)
            total = jnp.sum(weights[j].astype(jnp.float32), axis=1, keepdims=True)
            out = self.select(parts[j])
            self.num[row] = self.num[row] + out
            total = jnp.broadcast_to(total, out.shape)
            if self.per_device:
                lane = lax.broadcasted_iota(jnp.int32, out.shape, 1)
                total = jnp.where(lane == (row & (self.per_device - 1)), total, 0.0)
                row = row >> (self.per_device.bit_length() - 1)
            self.den[row] = self.den[row] + total

    def run(self, total, get_query):
        for j in range(GROUP):
            self.words[total + j] = 0

        @pl.when(total == 0)
        def _():
            self.start(0, 0, 0)
            self.words[0] = self.word(0, 0, 0)

        total = jnp.maximum(total, 1)
        self.total = total

        def rest(i, carry):
            self.start(i, self.slot(self.words[i]), 1)
            return carry

        lax.fori_loop(jnp.maximum(total - GROUP, 0), total, rest, 0)
        groups = (total + GROUP - 1) // GROUP
        self.wait(0, 0)
        weights = self.weights(0, self.scores(0, get_query))

        def step(g, weights):
            first = g * GROUP
            before = first - GROUP
            self.wait(first, 0)
            self.wait(before, 1)
            raws = self.scores(first, get_query)
            parts = self.products(before, weights)
            later = self.weights(first, raws)
            self.accumulate(before, weights, parts)
            return later

        weights = lax.fori_loop(1, groups, step, weights)
        last = (groups - 1) * GROUP
        self.wait(last, 1)
        self.accumulate(last, weights, self.products(last, weights))


def remote_kernel(
    n_heads, recv_ref, key_hbm, value_hbm, out_ref,
    meta, num, den, queries, words, key_buf, value_buf, sems,
):
    devices, tiles, part_rows = recv_ref.shape[:3]
    rows = out_ref.shape[2]
    n_dp = devices // n_heads
    parts = rows // part_rows
    capacity = (tiles - 1) // parts
    sessions = out_ref.shape[1] - 1
    page_size = key_hbm.shape[2]
    head = lax.axis_index("heads")
    for d in range(n_dp):
        meta[0, d : d + 1, :] = decode(recv_ref, d * n_heads + head)
        meta[1, d : d + 1, :] = longest_of(recv_ref, d, n_heads)
    own, longest = meta[0], meta[1]
    session = pltpu.roll(own, 128 - SESS_LANE, 1)
    page = pltpu.roll(own, 128 - PAGE_LANE, 1)
    length = jnp.zeros_like(own)
    for s in range(sessions):
        known = jnp.broadcast_to(longest[:, HIGH_LANE + s : HIGH_LANE + s + 1], own.shape)
        length = jnp.where(session == s, known, length)
    live = jnp.clip(length - page * page_size, 0, page_size)
    pages = Pages(key_hbm, value_hbm, words, key_buf, value_buf, sems, num, den, sessions)
    device = lax.broadcasted_iota(jnp.int32, own.shape, 0)
    asked = jnp.where(own > 0, pages.word(own - 1, live, device * sessions + session), 0)
    total = jnp.int32(0)
    for d in range(n_dp):
        for c in range(capacity):
            word = asked[d, c]
            for k in range(parts):
                queries[total, k * part_rows : (k + 1) * part_rows] = recv_ref[
                    d * n_heads + head, c * parts + k
                ]
            total = pages.add(total, word > 0, word)
    num[...] = jnp.zeros_like(num)
    den[...] = jnp.zeros_like(den)
    pages.run(total, lambda i: queries[i])

    for d in range(n_dp):
        for s in range(sessions):
            out_ref[d, s] = num[d * sessions + s].astype(jnp.bfloat16)
        high = den[d].astype(jnp.bfloat16).astype(jnp.float32)
        out_ref[d, sessions] = (high + pltpu.roll(den[d] - high, 64, 1)).astype(jnp.bfloat16)


def local_kernel(
    n_heads, recv_ref, table_hbm, plan_hbm, finished_hbm, query_hbm, key_hbm, value_hbm,
    num, den, table_ref, plan_ref, finished_ref, query_ref, loads,
    moved, words, key_buf, value_buf, sems,
):
    copies = load_all(
        [
            (table_hbm, table_ref),
            (plan_hbm, plan_ref),
            (finished_hbm, finished_ref),
            (query_hbm, query_ref),
        ],
        loads,
    )
    sessions, pages_max = table_ref.shape
    page_size = key_hbm.shape[2]
    slots = key_hbm.shape[0]
    longest = longest_of(recv_ref, lax.axis_index("dp"), n_heads)
    num[...] = jnp.zeros_like(num)
    for j in range(slots):
        moved[j] = 0
    for load in copies:
        load.wait()
    for s in range(sessions):
        den[s] = jnp.full(den.shape[1:], 1.0, jnp.float32) * finished_ref[0, s].astype(jnp.float32)
    for r in range(plan_ref.shape[1]):
        moved[plan_ref[2, r]] = 1
    pages = Pages(key_hbm, value_hbm, words, key_buf, value_buf, sems, num, den)
    total = jnp.int32(0)
    for s in range(sessions):
        length = jnp.where(finished_ref[0, s] == 1, 0, longest[0, HIGH_LANE + s])
        for p in range(pages_max):
            slot = table_ref[s, p]
            live = jnp.clip(length - p * page_size, 0, page_size)
            needed = (live > 0) & (moved[slot] == 0)
            total = pages.add(total, needed, pages.word(slot, live, s))
    pages.run(total, lambda i: query_ref[pages.row(i)])


def combine_kernel(back_ref, num_ref, den_ref, out_ref):
    n_dp, tiles, rows = back_ref.shape[:3]
    sessions = tiles - 1
    packed = back_ref[0, sessions].astype(jnp.float32)
    for d in range(1, n_dp):
        packed = packed + back_ref[d, sessions].astype(jnp.float32)
    packed = packed + pltpu.roll(packed, 64, 1)
    for s in range(sessions):
        total = num_ref[s]
        for d in range(n_dp):
            total = total + back_ref[d, s].astype(jnp.float32)
        weight = den_ref[s] + jnp.broadcast_to(packed[:, s : s + 1], (rows, 128))
        out_ref[s] = (total / weight).astype(jnp.bfloat16)


def body(queries, key_cache, value_cache, lengths_seen, page_table, finished, move_plan):
    slot_total, kv_heads, page_size, head_dim = key_cache.shape
    sessions, q_heads, _ = queries.shape
    pages_max = page_table.shape[1]
    moves = move_plan.shape[0]
    n_dp = lax.axis_size("dp")
    n_heads = lax.axis_size("heads")
    capacity = (moves - 1) // (n_dp - 1) + 1
    assert capacity <= 32 and sessions <= 16 and slot_total < 256 and pages_max <= 256
    assert page_size & (page_size - 1) == 0 and sessions & (sessions - 1) == 0
    assert n_dp * sessions << 8 << 10 < 2**31

    seen = in_hbm(lengths_seen.T)
    plan = in_hbm(move_plan.T)
    table = in_hbm(page_table)
    query = in_hbm(queries)
    done = in_hbm(finished.reshape(1, sessions))
    keys = in_hbm(key_cache)
    values = in_hbm(value_cache)

    packed = pl.pallas_call(
        functools.partial(pack_kernel, n_heads),
        out_shape=jax.ShapeDtypeStruct(
            (n_dp * n_heads, capacity * kv_heads + 1, q_heads // kv_heads, head_dim), jnp.bfloat16
        ),
        in_specs=[HBM] * 4,
        out_specs=VMEM,
        scratch_shapes=[
            pltpu.SMEM((1, sessions), jnp.int32),
            pltpu.SMEM((sessions, pages_max), jnp.int32),
            pltpu.SMEM(plan.shape, jnp.int32),
            pltpu.VMEM(queries.shape, queries.dtype),
            pltpu.SemaphoreType.DMA((4,)),
            pltpu.SMEM((slot_total,), jnp.int32),
            pltpu.SMEM((n_dp,), jnp.int32),
            pltpu.VMEM((n_dp, 1, 128), jnp.int32),
        ],
        compiler_params=pltpu.CompilerParams(vmem_limit_bytes=SMALL_VMEM),
        name="pack",
    )(seen, table, plan, query)
    recv = lax.all_to_all(packed, ("dp", "heads"), split_axis=0, concat_axis=0, tiled=True)

    def page_scratch(count):
        buffer = pltpu.VMEM((count, kv_heads, page_size, head_dim), jnp.bfloat16)
        return [
            pltpu.SMEM((count + GROUP,), jnp.int32),
            buffer,
            buffer,
            pltpu.SemaphoreType.DMA((2, count)),
        ]

    def page_limit(count):
        pages = 2 * count * kv_heads * page_size * head_dim * 2
        return pltpu.CompilerParams(vmem_limit_bytes=pages + SMALL_VMEM)

    asked = n_dp * capacity
    response = pl.pallas_call(
        functools.partial(remote_kernel, n_heads),
        out_shape=jax.ShapeDtypeStruct((n_dp, sessions + 1, q_heads, head_dim), jnp.bfloat16),
        in_specs=[VMEM, HBM, HBM],
        out_specs=VMEM,
        scratch_shapes=[
            pltpu.VMEM((2, n_dp, 128), jnp.int32),
            pltpu.VMEM((n_dp * sessions, q_heads, head_dim), jnp.float32),
            pltpu.VMEM((n_dp, q_heads, head_dim), jnp.float32),
            pltpu.VMEM((asked + GROUP, q_heads, head_dim), jnp.bfloat16),
            *page_scratch(asked),
        ],
        compiler_params=page_limit(asked),
        name="remote_pages",
        cost_estimate=pl.CostEstimate(flops=10**8, transcendentals=0, bytes_accessed=10**7),
    )(recv, keys, values)
    back = lax.all_to_all(response, "dp", split_axis=0, concat_axis=0, tiled=True)
    held = sessions * pages_max
    accumulator = jax.ShapeDtypeStruct((sessions, q_heads, head_dim), jnp.float32)
    num, den = pl.pallas_call(
        functools.partial(local_kernel, n_heads),
        out_shape=(accumulator, accumulator),
        in_specs=[VMEM, HBM, HBM, HBM, HBM, HBM, HBM],
        out_specs=(VMEM, VMEM),
        scratch_shapes=[
            pltpu.SMEM((sessions, pages_max), jnp.int32),
            pltpu.SMEM(plan.shape, jnp.int32),
            pltpu.SMEM((1, sessions), jnp.int32),
            pltpu.VMEM(queries.shape, queries.dtype),
            pltpu.SemaphoreType.DMA((4,)),
            pltpu.SMEM((slot_total,), jnp.int32),
            *page_scratch(held),
        ],
        compiler_params=page_limit(held),
        name="local_pages",
        cost_estimate=pl.CostEstimate(flops=10**9, transcendentals=0, bytes_accessed=10**7),
    )(recv, table, plan, done, query, keys, values)
    return pl.pallas_call(
        combine_kernel,
        out_shape=jax.ShapeDtypeStruct((sessions, q_heads, head_dim), jnp.bfloat16),
        in_specs=[VMEM, VMEM, VMEM],
        out_specs=VMEM,
        compiler_params=pltpu.CompilerParams(vmem_limit_bytes=SMALL_VMEM),
        name="combine",
    )(back, num, den)


def solution(mesh):
    in_specs = (
        P("dp", "heads", None),
        P("dp", "heads", None, None),
        P("dp", "heads", None, None),
        P("dp", "heads"),
        P("dp", None),
        P("dp"),
        P("dp", None),
    )
    out_specs = P("dp", "heads", None)
    return jax.shard_map(body, mesh=mesh, in_specs=in_specs, out_specs=out_specs, check_vma=False)
```

```python
import functools
import math

import jax
import jax.numpy as jnp
from jax import lax
from jax.experimental import pallas as pl
from jax.experimental.pallas import tpu as pltpu
from jax.sharding import PartitionSpec as P

softcap_limit = 50.0
score_divisor = 12.0
exp_scale = softcap_limit * math.log2(math.e)
GROUP = 5
LEN_BASE = 128
SMALL_VMEM = 4 << 20
SESS_LANE, PAGE_LANE, HIGH_LANE, LOW_LANE = 32, 64, 96, 112

VMEM = pl.BlockSpec(memory_space=pltpu.VMEM)
HBM = pl.BlockSpec(memory_space=pltpu.HBM)


def in_hbm(array):
    return pltpu.with_memory_space_constraint(array, pltpu.HBM)


def load_all(pairs, sems):
    copies = [pltpu.make_async_copy(s, d, sems.at[i]) for i, (s, d) in enumerate(pairs)]
    for copy in copies:
        copy.start()
    return copies


def pack_kernel(
    n_heads, len_hbm, table_hbm, plan_hbm, query_hbm, out_ref,
    len_ref, table_ref, plan_ref, query_ref, sems, owner, count, meta,
):
    copies = load_all(
        [(len_hbm, len_ref), (table_hbm, table_ref), (plan_hbm, plan_ref), (query_hbm, query_ref)],
        sems,
    )
    sessions, pages_max = table_ref.shape
    moves = plan_ref.shape[1]
    devices, tiles = out_ref.shape[:2]
    n_dp = devices // n_heads
    rows = out_ref.shape[2]
    parts = query_ref.shape[1] // rows
    head = lax.axis_index("heads")
    lane = lax.broadcasted_iota(jnp.int32, (1, 128), 1)
    base = jnp.zeros((1, 128), jnp.int32)
    for d in range(n_dp):
        count[d] = 0
    for copy in copies:
        copy.wait()
    for s in range(sessions):
        length = len_ref[0, s]
        base = jnp.where(lane == HIGH_LANE + s, length // LEN_BASE, base)
        base = jnp.where(lane == LOW_LANE + s, length % LEN_BASE, base)
        for p in range(pages_max):
            owner[table_ref[s, p]] = s * 256 + p
    for d in range(n_dp):
        meta[d] = base
    for r in range(moves):
        source = plan_ref[0, r]
        rank = count[source]
        count[source] = rank + 1
        entry = owner[plan_ref[2, r]]
        session = entry >> 8
        row = meta[source]
        row = jnp.where(lane == rank, plan_ref[1, r] + 1, row)
        row = jnp.where(lane == SESS_LANE + rank, session, row)
        row = jnp.where(lane == PAGE_LANE + rank, entry & 255, row)
        meta[source] = row
        tile = query_ref[session]
        for k in range(parts):
            out_ref[source * n_heads + head, rank * parts + k] = tile[k * rows : (k + 1) * rows]
    for d in range(n_dp):
        row = jnp.broadcast_to(meta[d].astype(jnp.float32), (rows, 128)).astype(jnp.bfloat16)
        for h in range(n_heads):
            out_ref[d * n_heads + h, tiles - 1] = row


def decode(recv_ref, index):
    tile = recv_ref[index, recv_ref.shape[1] - 1]
    return tile.astype(jnp.float32).astype(jnp.int32)[0:1]


def longest_of(recv_ref, d, n_heads):
    longest = None
    for h in range(n_heads):
        block = decode(recv_ref, d * n_heads + h)
        length = block * LEN_BASE + pltpu.roll(block, 128 - (LOW_LANE - HIGH_LANE), 1)
        longest = length if longest is None else jnp.maximum(longest, length)
    return longest


class Pages:
    def __init__(
        self, key_hbm, value_hbm, words, key_buf, value_buf, sems, num, den, per_device=None
    ):
        self.key_hbm, self.value_hbm, self.words = key_hbm, value_hbm, words
        self.key_buf, self.value_buf, self.sems = key_buf, value_buf, sems
        self.num, self.den, self.per_device = num, den, per_device
        self.kv_heads, self.page_size = key_hbm.shape[1:3]
        self.rows = num.shape[1]
        self.group = self.rows // self.kv_heads
        self.live_shift = key_hbm.shape[0].bit_length()
        self.row_shift = self.live_shift + self.page_size.bit_length()

    def word(self, slot, live, row):
        return (slot + 1) + live * (1 << self.live_shift) + row * (1 << self.row_shift)

    def slot(self, word):
        return (word & ((1 << self.live_shift) - 1)) - 1

    def live(self, i):
        return (self.words[i] >> self.live_shift) & (2 * self.page_size - 1)

    def row(self, i):
        return self.words[i] >> self.row_shift

    def buffer(self, i):
        return jnp.minimum(i, self.total - 1)

    def start(self, i, slot, which):
        buf, hbm = (self.key_buf, self.key_hbm) if which == 0 else (self.value_buf, self.value_hbm)
        pltpu.make_async_copy(hbm.at[slot], buf.at[i], self.sems.at[which, i]).start()

    def add(self, total, needed, word):
        @pl.when(needed)
        def _():
            self.start(total, self.slot(word), 0)
            self.words[total] = word

        @pl.when(needed & (total >= GROUP))
        def _():
            before = total - GROUP
            self.start(before, self.slot(self.words[before]), 1)

        return total + needed.astype(jnp.int32)

    def wait(self, first, which):
        buf, hbm = (self.key_buf, self.key_hbm) if which == 0 else (self.value_buf, self.value_hbm)
        for j in range(GROUP):
            i = first + j

            @pl.when(i < self.total)
            def _(i=i):
                pltpu.make_async_copy(hbm.at[0], buf.at[i], self.sems.at[which, i]).wait()

    def scores(self, first, get_query):
        raws = []
        for j in range(GROUP):
            i = first + j
            query = get_query(i)
            buffer = self.buffer(i)
            raws.append(
                [
                    lax.dot_general(
                        query,
                        self.key_buf[buffer, k],
                        (((1,), (1,)), ((), ())),
                        preferred_element_type=jnp.float32,
                    )
                    for k in range(self.kv_heads)
                ]
            )
        return raws

    def select(self, parts):
        row = lax.broadcasted_iota(jnp.int32, parts[0].shape, 0)
        out = parts[-1]
        for k in reversed(range(self.kv_heads - 1)):
            out = jnp.where(row < (k + 1) * self.group, parts[k], out)
        return out

    def weights(self, first, raws):
        out = []
        place = lax.broadcasted_iota(jnp.int32, (self.rows, self.page_size), 1)
        for j in range(GROUP):
            raw = self.select(raws[j])
            capped = jnp.tanh(raw * (1.0 / (score_divisor * softcap_limit)))
            weight = jnp.exp2(capped * exp_scale)
            live = self.live(first + j)
            out.append(jnp.where(place < live, weight, 0.0).astype(jnp.bfloat16))
        return out

    def products(self, first, weights):
        parts = []
        for j in range(GROUP):
            buffer = self.buffer(first + j)
            parts.append(
                [
                    jnp.dot(
                        weights[j], self.value_buf[buffer, k], preferred_element_type=jnp.float32
                    )
                    for k in range(self.kv_heads)
                ]
            )
        return parts

    def accumulate(self, first, weights, parts):
        for j in range(GROUP):
            row = self.row(first + j)
            total = jnp.sum(weights[j].astype(jnp.float32), axis=1, keepdims=True)
            out = self.select(parts[j])
            self.num[row] = self.num[row] + out
            total = jnp.broadcast_to(total, out.shape)
            if self.per_device:
                lane = lax.broadcasted_iota(jnp.int32, out.shape, 1)
                total = jnp.where(lane == (row & (self.per_device - 1)), total, 0.0)
                row = row >> (self.per_device.bit_length() - 1)
            self.den[row] = self.den[row] + total

    def run(self, total, get_query):
        for j in range(GROUP):
            self.words[total + j] = 0

        @pl.when(total == 0)
        def _():
            self.start(0, 0, 0)
            self.words[0] = self.word(0, 0, 0)

        total = jnp.maximum(total, 1)
        self.total = total

        def rest(i, carry):
            self.start(i, self.slot(self.words[i]), 1)
            return carry

        lax.fori_loop(jnp.maximum(total - GROUP, 0), total, rest, 0)
        groups = (total + GROUP - 1) // GROUP
        self.wait(0, 0)
        weights = self.weights(0, self.scores(0, get_query))

        def step(g, weights):
            first = g * GROUP
            before = first - GROUP
            self.wait(first, 0)
            self.wait(before, 1)
            raws = self.scores(first, get_query)
            parts = self.products(before, weights)
            later = self.weights(first, raws)
            self.accumulate(before, weights, parts)
            return later

        weights = lax.fori_loop(1, groups, step, weights)
        last = (groups - 1) * GROUP
        self.wait(last, 1)
        self.accumulate(last, weights, self.products(last, weights))


def remote_kernel(
    n_heads, sessions, recv_ref, key_hbm, value_hbm, out_ref,
    meta, num, den, queries, words, key_buf, value_buf, sems,
):
    devices, tiles, part_rows = recv_ref.shape[:3]
    rows = num.shape[1]
    n_dp = devices // n_heads
    parts = rows // part_rows
    capacity = (tiles - 1) // parts
    places = num.shape[0] // n_dp
    page_size = key_hbm.shape[2]
    head = lax.axis_index("heads")
    for d in range(n_dp):
        meta[0, d : d + 1, :] = decode(recv_ref, d * n_heads + head)
        meta[1, d : d + 1, :] = longest_of(recv_ref, d, n_heads)
    own, longest = meta[0], meta[1]
    session = pltpu.roll(own, 128 - SESS_LANE, 1)
    page = pltpu.roll(own, 128 - PAGE_LANE, 1)
    length = jnp.zeros_like(own)
    for s in range(sessions):
        known = jnp.broadcast_to(longest[:, HIGH_LANE + s : HIGH_LANE + s + 1], own.shape)
        length = jnp.where(session == s, known, length)
    live = jnp.clip(length - page * page_size, 0, page_size)
    pages = Pages(key_hbm, value_hbm, words, key_buf, value_buf, sems, num, den, places)
    device = lax.broadcasted_iota(jnp.int32, own.shape, 0)
    place = lax.broadcasted_iota(jnp.int32, own.shape, 1) & (places - 1)
    asked = jnp.where(own > 0, pages.word(own - 1, live, device * places + place), 0)
    total = jnp.int32(0)
    for d in range(n_dp):
        for c in range(capacity):
            word = asked[d, c]
            for k in range(parts):
                queries[total, k * part_rows : (k + 1) * part_rows] = recv_ref[
                    d * n_heads + head, c * parts + k
                ]
            total = pages.add(total, word > 0, word)
    num[...] = jnp.zeros_like(num)
    den[...] = jnp.zeros_like(den)
    pages.run(total, lambda i: queries[i])

    for d in range(n_dp):
        for c in range(capacity):
            out_ref[d, c * rows : (c + 1) * rows] = num[d * places + c].astype(jnp.bfloat16)
        high = den[d].astype(jnp.bfloat16).astype(jnp.float32)
        used = (capacity + 1) * rows
        out_ref[d, used - rows : used] = (high + pltpu.roll(den[d] - high, 64, 1)).astype(
            jnp.bfloat16
        )
        if used < out_ref.shape[1]:
            out_ref[d, used:] = jnp.zeros((out_ref.shape[1] - used, 128), jnp.bfloat16)


def local_kernel(
    n_heads, recv_ref, table_hbm, plan_hbm, finished_hbm, query_hbm, key_hbm, value_hbm,
    num, den, spread_ref, place_ref, table_ref, plan_ref, finished_ref, query_ref, loads,
    moved, owner, count, words, key_buf, value_buf, sems,
):
    copies = load_all(
        [
            (table_hbm, table_ref),
            (plan_hbm, plan_ref),
            (finished_hbm, finished_ref),
            (query_hbm, query_ref),
        ],
        loads,
    )
    sessions, pages_max = table_ref.shape
    page_size = key_hbm.shape[2]
    slots = key_hbm.shape[0]
    longest = longest_of(recv_ref, lax.axis_index("dp"), n_heads)
    num[...] = jnp.zeros_like(num)
    for j in range(slots):
        moved[j] = 0
    for load in copies:
        load.wait()
    for s in range(sessions):
        den[s] = jnp.full(den.shape[1:], 1.0, jnp.float32) * finished_ref[0, s].astype(jnp.float32)
    for r in range(plan_ref.shape[1]):
        moved[plan_ref[2, r]] = 1
    pages = Pages(key_hbm, value_hbm, words, key_buf, value_buf, sems, num, den)
    total = jnp.int32(0)
    for s in range(sessions):
        length = jnp.where(finished_ref[0, s] == 1, 0, longest[0, HIGH_LANE + s])
        for p in range(pages_max):
            slot = table_ref[s, p]
            live = jnp.clip(length - p * page_size, 0, page_size)
            needed = (live > 0) & (moved[slot] == 0)
            total = pages.add(total, needed, pages.word(slot, live, s))
    pages.run(total, lambda i: query_ref[pages.row(i)])

    n_dp = place_ref.shape[0]
    rows = num.shape[1]
    stride = spread_ref.shape[1] // n_dp
    for s in range(sessions):
        for p in range(pages_max):
            owner[table_ref[s, p]] = s
    for d in range(n_dp):
        count[d] = 0
    row = lax.broadcasted_iota(jnp.int32, spread_ref.shape, 0)
    column = lax.broadcasted_iota(jnp.int32, spread_ref.shape, 1)
    device = lax.broadcasted_iota(jnp.int32, place_ref.shape, 0)
    lane = lax.broadcasted_iota(jnp.int32, place_ref.shape, 1) & 63
    session_row = row // rows
    spread = jnp.zeros(spread_ref.shape, jnp.float32)
    places = jnp.full(place_ref.shape, -1, jnp.int32)
    for r in range(plan_ref.shape[1]):
        source = plan_ref[0, r]
        rank = count[source]
        count[source] = rank + 1
        session = owner[plan_ref[2, r]]
        offset = source * stride + rank * rows - session * rows
        spread = jnp.where((column - row == offset) & (session_row == session), 1.0, spread)
        places = jnp.where((device == source) & (lane == rank), session, places)
    spread_ref[...] = spread.astype(jnp.bfloat16)
    place_ref[...] = places


def combine_kernel(capacity, back_ref, num_ref, den_ref, spread_ref, place_ref, out_ref):
    n_dp, stride = back_ref.shape[:2]
    sessions, rows = num_ref.shape[:2]
    moved = jnp.dot(
        spread_ref[...],
        back_ref[...].reshape(n_dp * stride, 128),
        preferred_element_type=jnp.float32,
    )
    tile = slice(capacity * rows, (capacity + 1) * rows)
    weights = [back_ref[d, tile].astype(jnp.float32) for d in range(n_dp)]
    for s in range(sessions):
        packed = jnp.zeros((rows, 128), jnp.float32)
        for d in range(n_dp):
            mine = jnp.broadcast_to(place_ref[d : d + 1, :], (rows, 128)) == s
            packed = packed + jnp.where(mine, weights[d], 0.0)
        weight = den_ref[s] + jnp.sum(packed, axis=1, keepdims=True)
        total = num_ref[s] + moved[s * rows : (s + 1) * rows]
        out_ref[s] = (total / weight).astype(jnp.bfloat16)


def body(queries, key_cache, value_cache, lengths_seen, page_table, finished, move_plan):
    slot_total, kv_heads, page_size, head_dim = key_cache.shape
    sessions, q_heads, _ = queries.shape
    pages_max = page_table.shape[1]
    moves = move_plan.shape[0]
    n_dp = lax.axis_size("dp")
    n_heads = lax.axis_size("heads")
    capacity = (moves - 1) // (n_dp - 1) + 1
    assert capacity <= 32 and sessions <= 16 and slot_total < 256 and pages_max <= 256
    assert page_size & (page_size - 1) == 0 and sessions & (sessions - 1) == 0
    assert n_dp * sessions << 8 << 10 < 2**31

    seen = in_hbm(lengths_seen.T)
    plan = in_hbm(move_plan.T)
    table = in_hbm(page_table)
    query = in_hbm(queries)
    done = in_hbm(finished.reshape(1, sessions))
    keys = in_hbm(key_cache)
    values = in_hbm(value_cache)

    packed = pl.pallas_call(
        functools.partial(pack_kernel, n_heads),
        out_shape=jax.ShapeDtypeStruct(
            (n_dp * n_heads, capacity * kv_heads + 1, q_heads // kv_heads, head_dim), jnp.bfloat16
        ),
        in_specs=[HBM] * 4,
        out_specs=VMEM,
        scratch_shapes=[
            pltpu.SMEM((1, sessions), jnp.int32),
            pltpu.SMEM((sessions, pages_max), jnp.int32),
            pltpu.SMEM(plan.shape, jnp.int32),
            pltpu.VMEM(queries.shape, queries.dtype),
            pltpu.SemaphoreType.DMA((4,)),
            pltpu.SMEM((slot_total,), jnp.int32),
            pltpu.SMEM((n_dp,), jnp.int32),
            pltpu.VMEM((n_dp, 1, 128), jnp.int32),
        ],
        compiler_params=pltpu.CompilerParams(vmem_limit_bytes=SMALL_VMEM),
        name="pack",
    )(seen, table, plan, query)
    recv = lax.all_to_all(packed, ("dp", "heads"), split_axis=0, concat_axis=0, tiled=True)

    def page_scratch(count):
        buffer = pltpu.VMEM((count, kv_heads, page_size, head_dim), jnp.bfloat16)
        return [
            pltpu.SMEM((count + GROUP,), jnp.int32),
            buffer,
            buffer,
            pltpu.SemaphoreType.DMA((2, count)),
        ]

    def page_limit(count):
        pages = 2 * count * kv_heads * page_size * head_dim * 2
        return pltpu.CompilerParams(vmem_limit_bytes=pages + SMALL_VMEM)

    asked = n_dp * capacity
    places = 1 << (capacity - 1).bit_length()
    stride = -(-(capacity + 1) * q_heads // 8) * 8
    response = pl.pallas_call(
        functools.partial(remote_kernel, n_heads, sessions),
        out_shape=jax.ShapeDtypeStruct((n_dp, stride, head_dim), jnp.bfloat16),
        in_specs=[VMEM, HBM, HBM],
        out_specs=VMEM,
        scratch_shapes=[
            pltpu.VMEM((2, n_dp, 128), jnp.int32),
            pltpu.VMEM((n_dp * places, q_heads, head_dim), jnp.float32),
            pltpu.VMEM((n_dp, q_heads, head_dim), jnp.float32),
            pltpu.VMEM((asked + GROUP, q_heads, head_dim), jnp.bfloat16),
            *page_scratch(asked),
        ],
        compiler_params=page_limit(asked),
        name="remote_pages",
        cost_estimate=pl.CostEstimate(flops=10**8, transcendentals=0, bytes_accessed=10**7),
    )(recv, keys, values)
    back = lax.all_to_all(response, "dp", split_axis=0, concat_axis=0, tiled=True)
    held = sessions * pages_max
    accumulator = jax.ShapeDtypeStruct((sessions, q_heads, head_dim), jnp.float32)
    num, den, spread, place = pl.pallas_call(
        functools.partial(local_kernel, n_heads),
        out_shape=(
            accumulator,
            accumulator,
            jax.ShapeDtypeStruct((sessions * q_heads, n_dp * stride), jnp.bfloat16),
            jax.ShapeDtypeStruct((n_dp, 128), jnp.int32),
        ),
        in_specs=[VMEM, HBM, HBM, HBM, HBM, HBM, HBM],
        out_specs=(VMEM,) * 4,
        scratch_shapes=[
            pltpu.SMEM((sessions, pages_max), jnp.int32),
            pltpu.SMEM(plan.shape, jnp.int32),
            pltpu.SMEM((1, sessions), jnp.int32),
            pltpu.VMEM(queries.shape, queries.dtype),
            pltpu.SemaphoreType.DMA((4,)),
            pltpu.SMEM((slot_total,), jnp.int32),
            pltpu.SMEM((slot_total,), jnp.int32),
            pltpu.SMEM((n_dp,), jnp.int32),
            *page_scratch(held),
        ],
        compiler_params=page_limit(held),
        name="local_pages",
        cost_estimate=pl.CostEstimate(flops=10**9, transcendentals=0, bytes_accessed=10**7),
    )(recv, table, plan, done, query, keys, values)
    return pl.pallas_call(
        functools.partial(combine_kernel, capacity),
        out_shape=jax.ShapeDtypeStruct((sessions, q_heads, head_dim), jnp.bfloat16),
        in_specs=[VMEM] * 5,
        out_specs=VMEM,
        compiler_params=pltpu.CompilerParams(vmem_limit_bytes=SMALL_VMEM),
        name="combine",
    )(back, num, den, spread, place)


def solution(mesh):
    in_specs = (
        P("dp", "heads", None),
        P("dp", "heads", None, None),
        P("dp", "heads", None, None),
        P("dp", "heads"),
        P("dp", None),
        P("dp"),
        P("dp", None),
    )
    out_specs = P("dp", "heads", None)
    return jax.shard_map(body, mesh=mesh, in_specs=in_specs, out_specs=out_specs, check_vma=False)
```

```python
import functools
import math

import jax
import jax.numpy as jnp
from jax import lax
from jax.experimental import pallas as pl
from jax.experimental.pallas import tpu as pltpu
from jax.sharding import PartitionSpec as P

softcap_limit = 50.0
score_divisor = 12.0
exp_scale = softcap_limit * math.log2(math.e)
GROUP = 5
LEN_BASE = 128
SMALL_VMEM = 4 << 20
SESS_LANE, PAGE_LANE, HIGH_LANE, LOW_LANE = 32, 64, 96, 112

VMEM = pl.BlockSpec(memory_space=pltpu.VMEM)
HBM = pl.BlockSpec(memory_space=pltpu.HBM)


def in_hbm(array):
    return pltpu.with_memory_space_constraint(array, pltpu.HBM)


def load_all(pairs, sems):
    copies = [pltpu.make_async_copy(s, d, sems.at[i]) for i, (s, d) in enumerate(pairs)]
    for copy in copies:
        copy.start()
    return copies


def pack_kernel(
    n_heads, len_hbm, table_hbm, plan_hbm, query_hbm, out_ref,
    len_ref, table_ref, plan_ref, query_ref, sems, owner, count, meta,
):
    copies = load_all(
        [(len_hbm, len_ref), (table_hbm, table_ref), (plan_hbm, plan_ref), (query_hbm, query_ref)],
        sems,
    )
    sessions, pages_max = table_ref.shape
    moves = plan_ref.shape[1]
    devices, tiles = out_ref.shape[:2]
    n_dp = devices // n_heads
    rows = out_ref.shape[2]
    parts = query_ref.shape[1] // rows
    head = lax.axis_index("heads")
    lane = lax.broadcasted_iota(jnp.int32, (1, 128), 1)
    base = jnp.zeros((1, 128), jnp.int32)
    for d in range(n_dp):
        count[d] = 0
    for copy in copies:
        copy.wait()
    for s in range(sessions):
        length = len_ref[0, s]
        base = jnp.where(lane == HIGH_LANE + s, length // LEN_BASE, base)
        base = jnp.where(lane == LOW_LANE + s, length % LEN_BASE, base)
        for p in range(pages_max):
            owner[table_ref[s, p]] = s * 256 + p
    for d in range(n_dp):
        meta[d] = base
    for r in range(moves):
        source = plan_ref[0, r]
        rank = count[source]
        count[source] = rank + 1
        entry = owner[plan_ref[2, r]]
        session = entry >> 8
        row = meta[source]
        row = jnp.where(lane == rank, plan_ref[1, r] + 1, row)
        row = jnp.where(lane == SESS_LANE + rank, session, row)
        row = jnp.where(lane == PAGE_LANE + rank, entry & 255, row)
        meta[source] = row
        tile = query_ref[session]
        for k in range(parts):
            out_ref[source * n_heads + head, rank * parts + k] = tile[k * rows : (k + 1) * rows]
    for d in range(n_dp):
        row = jnp.broadcast_to(meta[d].astype(jnp.float32), (rows, 128)).astype(jnp.bfloat16)
        for h in range(n_heads):
            out_ref[d * n_heads + h, tiles - 1] = row


def decode(recv_ref, index):
    tile = recv_ref[index, recv_ref.shape[1] - 1]
    return tile.astype(jnp.float32).astype(jnp.int32)[0:1]


def longest_of(recv_ref, d, n_heads):
    longest = None
    for h in range(n_heads):
        block = decode(recv_ref, d * n_heads + h)
        length = block * LEN_BASE + pltpu.roll(block, 128 - (LOW_LANE - HIGH_LANE), 1)
        longest = length if longest is None else jnp.maximum(longest, length)
    return longest


class Pages:
    def __init__(
        self, key_hbm, value_hbm, words, key_buf, value_buf, sems, num, den, per_device=None,
        lives=None,
    ):
        self.key_hbm, self.value_hbm, self.words = key_hbm, value_hbm, words
        self.key_buf, self.value_buf, self.sems = key_buf, value_buf, sems
        self.num, self.den, self.per_device, self.lives = num, den, per_device, lives
        self.kv_heads, self.page_size = key_hbm.shape[1:3]
        self.rows = num.shape[1]
        self.group = self.rows // self.kv_heads
        self.live_shift = key_hbm.shape[0].bit_length()
        self.row_shift = self.live_shift + self.page_size.bit_length()

    def word(self, slot, live, row):
        return (slot + 1) + live * (1 << self.live_shift) + row * (1 << self.row_shift)

    def slot(self, word):
        return (word & ((1 << self.live_shift) - 1)) - 1

    def live(self, i):
        if self.lives is not None:
            return jnp.where(self.words[i] > 0, self.lives[self.row(i)], 0)
        return (self.words[i] >> self.live_shift) & (2 * self.page_size - 1)

    def row(self, i):
        return self.words[i] >> self.row_shift

    def buffer(self, i):
        return jnp.minimum(i, self.total - 1)

    def start(self, i, slot, which):
        buf, hbm = (self.key_buf, self.key_hbm) if which == 0 else (self.value_buf, self.value_hbm)
        pltpu.make_async_copy(hbm.at[slot], buf.at[i], self.sems.at[which, i]).start()

    def add(self, total, needed, word):
        @pl.when(needed)
        def _():
            self.start(total, self.slot(word), 0)
            self.words[total] = word

        @pl.when(needed & (total >= GROUP))
        def _():
            before = total - GROUP
            self.start(before, self.slot(self.words[before]), 1)

        return total + needed.astype(jnp.int32)

    def wait(self, first, which):
        buf, hbm = (self.key_buf, self.key_hbm) if which == 0 else (self.value_buf, self.value_hbm)
        for j in range(GROUP):
            i = first + j

            @pl.when(i < self.total)
            def _(i=i):
                pltpu.make_async_copy(hbm.at[0], buf.at[i], self.sems.at[which, i]).wait()

    def scores(self, first, get_query):
        raws = []
        for j in range(GROUP):
            i = first + j
            query = get_query(i)
            buffer = self.buffer(i)
            raws.append(
                [
                    lax.dot_general(
                        query,
                        self.key_buf[buffer, k],
                        (((1,), (1,)), ((), ())),
                        preferred_element_type=jnp.float32,
                    )
                    for k in range(self.kv_heads)
                ]
            )
        return raws

    def select(self, parts):
        row = lax.broadcasted_iota(jnp.int32, parts[0].shape, 0)
        out = parts[-1]
        for k in reversed(range(self.kv_heads - 1)):
            out = jnp.where(row < (k + 1) * self.group, parts[k], out)
        return out

    def weights(self, first, raws):
        out = []
        place = lax.broadcasted_iota(jnp.int32, (self.rows, self.page_size), 1)
        for j in range(GROUP):
            raw = self.select(raws[j])
            capped = jnp.tanh(raw * (1.0 / (score_divisor * softcap_limit)))
            weight = jnp.exp2(capped * exp_scale)
            live = self.live(first + j)
            out.append(jnp.where(place < live, weight, 0.0).astype(jnp.bfloat16))
        return out

    def products(self, first, weights):
        parts = []
        for j in range(GROUP):
            buffer = self.buffer(first + j)
            parts.append(
                [
                    jnp.dot(
                        weights[j], self.value_buf[buffer, k], preferred_element_type=jnp.float32
                    )
                    for k in range(self.kv_heads)
                ]
            )
        return parts

    def accumulate(self, first, weights, parts):
        for j in range(GROUP):
            row = self.row(first + j)
            total = jnp.sum(weights[j].astype(jnp.float32), axis=1, keepdims=True)
            out = self.select(parts[j])
            self.num[row] = self.num[row] + out
            total = jnp.broadcast_to(total, out.shape)
            if self.per_device:
                lane = lax.broadcasted_iota(jnp.int32, out.shape, 1)
                total = jnp.where(lane == (row & (self.per_device - 1)), total, 0.0)
                row = row >> (self.per_device.bit_length() - 1)
            self.den[row] = self.den[row] + total

    def run(self, total, get_query):
        for j in range(GROUP):
            self.words[total + j] = 0

        @pl.when(total == 0)
        def _():
            self.start(0, 0, 0)
            self.words[0] = self.word(0, 0, 0)

        total = jnp.maximum(total, 1)
        self.total = total

        def rest(i, carry):
            self.start(i, self.slot(self.words[i]), 1)
            return carry

        lax.fori_loop(jnp.maximum(total - GROUP, 0), total, rest, 0)
        groups = (total + GROUP - 1) // GROUP
        self.wait(0, 0)
        weights = self.weights(0, self.scores(0, get_query))

        def step(g, weights):
            first = g * GROUP
            before = first - GROUP
            self.wait(first, 0)
            self.wait(before, 1)
            raws = self.scores(first, get_query)
            parts = self.products(before, weights)
            later = self.weights(first, raws)
            self.accumulate(before, weights, parts)
            return later

        weights = lax.fori_loop(1, groups, step, weights)
        last = (groups - 1) * GROUP
        self.wait(last, 1)
        self.accumulate(last, weights, self.products(last, weights))


def remote_kernel(
    n_heads, sessions, recv_ref, key_hbm, value_hbm, out_ref,
    meta, num, den, queries, lives, words, key_buf, value_buf, sems,
):
    devices, tiles, part_rows = recv_ref.shape[:3]
    rows = num.shape[1]
    n_dp = devices // n_heads
    parts = rows // part_rows
    capacity = (tiles - 1) // parts
    places = num.shape[0] // n_dp
    page_size = key_hbm.shape[2]
    head = lax.axis_index("heads")
    for d in range(n_dp):
        meta[0, d : d + 1, :] = decode(recv_ref, d * n_heads + head)
    own = meta[0]
    pages = Pages(
        key_hbm, value_hbm, words, key_buf, value_buf, sems, num, den, places, lives
    )
    total = jnp.int32(0)
    for d in range(n_dp):
        for c in range(capacity):
            slot = own[d, c]
            for k in range(parts):
                queries[total, k * part_rows : (k + 1) * part_rows] = recv_ref[
                    d * n_heads + head, c * parts + k
                ]
            total = pages.add(total, slot > 0, pages.word(slot - 1, 0, d * places + c))

    for d in range(n_dp):
        meta[1, d : d + 1, :] = longest_of(recv_ref, d, n_heads)
    longest = meta[1]
    session = pltpu.roll(own, 128 - SESS_LANE, 1)
    page = pltpu.roll(own, 128 - PAGE_LANE, 1)
    length = jnp.zeros_like(own)
    for s in range(sessions):
        known = jnp.broadcast_to(longest[:, HIGH_LANE + s : HIGH_LANE + s + 1], own.shape)
        length = jnp.where(session == s, known, length)
    live = jnp.where(own > 0, jnp.clip(length - page * page_size, 0, page_size), 0)
    for d in range(n_dp):
        for c in range(capacity):
            lives[d * places + c] = live[d, c]
    num[...] = jnp.zeros_like(num)
    den[...] = jnp.zeros_like(den)
    pages.run(total, lambda i: queries[i])

    for d in range(n_dp):
        for c in range(capacity):
            out_ref[d, c * rows : (c + 1) * rows] = num[d * places + c].astype(jnp.bfloat16)
        high = den[d].astype(jnp.bfloat16).astype(jnp.float32)
        used = (capacity + 1) * rows
        out_ref[d, used - rows : used] = (high + pltpu.roll(den[d] - high, 64, 1)).astype(
            jnp.bfloat16
        )
        if used < out_ref.shape[1]:
            out_ref[d, used:] = jnp.zeros((out_ref.shape[1] - used, 128), jnp.bfloat16)


def local_kernel(
    n_heads, recv_ref, table_hbm, plan_hbm, finished_hbm, query_hbm, key_hbm, value_hbm,
    num, den, spread_ref, place_ref, table_ref, plan_ref, finished_ref, query_ref, loads,
    moved, owner, count, words, key_buf, value_buf, sems,
):
    copies = load_all(
        [
            (table_hbm, table_ref),
            (plan_hbm, plan_ref),
            (finished_hbm, finished_ref),
            (query_hbm, query_ref),
        ],
        loads,
    )
    sessions, pages_max = table_ref.shape
    page_size = key_hbm.shape[2]
    slots = key_hbm.shape[0]
    longest = longest_of(recv_ref, lax.axis_index("dp"), n_heads)
    num[...] = jnp.zeros_like(num)
    for j in range(slots):
        moved[j] = 0
    for load in copies:
        load.wait()
    for s in range(sessions):
        den[s] = jnp.full(den.shape[1:], 1.0, jnp.float32) * finished_ref[0, s].astype(jnp.float32)
    for r in range(plan_ref.shape[1]):
        moved[plan_ref[2, r]] = 1
    pages = Pages(key_hbm, value_hbm, words, key_buf, value_buf, sems, num, den)
    total = jnp.int32(0)
    for s in range(sessions):
        length = jnp.where(finished_ref[0, s] == 1, 0, longest[0, HIGH_LANE + s])
        for p in range(pages_max):
            slot = table_ref[s, p]
            live = jnp.clip(length - p * page_size, 0, page_size)
            needed = (live > 0) & (moved[slot] == 0)
            total = pages.add(total, needed, pages.word(slot, live, s))
    pages.run(total, lambda i: query_ref[pages.row(i)])

    n_dp = place_ref.shape[0]
    rows = num.shape[1]
    stride = spread_ref.shape[1] // n_dp
    for s in range(sessions):
        for p in range(pages_max):
            owner[table_ref[s, p]] = s
    for d in range(n_dp):
        count[d] = 0
    row = lax.broadcasted_iota(jnp.int32, spread_ref.shape, 0)
    column = lax.broadcasted_iota(jnp.int32, spread_ref.shape, 1)
    device = lax.broadcasted_iota(jnp.int32, place_ref.shape, 0)
    lane = lax.broadcasted_iota(jnp.int32, place_ref.shape, 1) & 63
    session_row = row // rows
    spread = jnp.zeros(spread_ref.shape, jnp.float32)
    places = jnp.full(place_ref.shape, -1, jnp.int32)
    for r in range(plan_ref.shape[1]):
        source = plan_ref[0, r]
        rank = count[source]
        count[source] = rank + 1
        session = owner[plan_ref[2, r]]
        offset = source * stride + rank * rows - session * rows
        spread = jnp.where((column - row == offset) & (session_row == session), 1.0, spread)
        places = jnp.where((device == source) & (lane == rank), session, places)
    spread_ref[...] = spread.astype(jnp.bfloat16)
    place_ref[...] = places


def combine_kernel(capacity, back_ref, num_ref, den_ref, spread_ref, place_ref, out_ref):
    n_dp, stride = back_ref.shape[:2]
    sessions, rows = num_ref.shape[:2]
    moved = jnp.dot(
        spread_ref[...],
        back_ref[...].reshape(n_dp * stride, 128),
        preferred_element_type=jnp.float32,
    )
    tile = slice(capacity * rows, (capacity + 1) * rows)
    weights = [back_ref[d, tile].astype(jnp.float32) for d in range(n_dp)]
    for s in range(sessions):
        packed = jnp.zeros((rows, 128), jnp.float32)
        for d in range(n_dp):
            mine = jnp.broadcast_to(place_ref[d : d + 1, :], (rows, 128)) == s
            packed = packed + jnp.where(mine, weights[d], 0.0)
        weight = den_ref[s] + jnp.sum(packed, axis=1, keepdims=True)
        total = num_ref[s] + moved[s * rows : (s + 1) * rows]
        out_ref[s] = (total / weight).astype(jnp.bfloat16)


def body(queries, key_cache, value_cache, lengths_seen, page_table, finished, move_plan):
    slot_total, kv_heads, page_size, head_dim = key_cache.shape
    sessions, q_heads, _ = queries.shape
    pages_max = page_table.shape[1]
    moves = move_plan.shape[0]
    n_dp = lax.axis_size("dp")
    n_heads = lax.axis_size("heads")
    capacity = (moves - 1) // (n_dp - 1) + 1
    assert capacity <= 32 and sessions <= 16 and slot_total < 256 and pages_max <= 256
    assert page_size & (page_size - 1) == 0 and sessions & (sessions - 1) == 0
    assert n_dp * sessions << 8 << 10 < 2**31

    seen = in_hbm(lengths_seen.T)
    plan = in_hbm(move_plan.T)
    table = in_hbm(page_table)
    query = in_hbm(queries)
    done = in_hbm(finished.reshape(1, sessions))
    keys = in_hbm(key_cache)
    values = in_hbm(value_cache)

    packed = pl.pallas_call(
        functools.partial(pack_kernel, n_heads),
        out_shape=jax.ShapeDtypeStruct(
            (n_dp * n_heads, capacity * kv_heads + 1, q_heads // kv_heads, head_dim), jnp.bfloat16
        ),
        in_specs=[HBM] * 4,
        out_specs=VMEM,
        scratch_shapes=[
            pltpu.SMEM((1, sessions), jnp.int32),
            pltpu.SMEM((sessions, pages_max), jnp.int32),
            pltpu.SMEM(plan.shape, jnp.int32),
            pltpu.VMEM(queries.shape, queries.dtype),
            pltpu.SemaphoreType.DMA((4,)),
            pltpu.SMEM((slot_total,), jnp.int32),
            pltpu.SMEM((n_dp,), jnp.int32),
            pltpu.VMEM((n_dp, 1, 128), jnp.int32),
        ],
        compiler_params=pltpu.CompilerParams(vmem_limit_bytes=SMALL_VMEM),
        name="pack",
    )(seen, table, plan, query)
    recv = lax.all_to_all(packed, ("dp", "heads"), split_axis=0, concat_axis=0, tiled=True)

    def page_scratch(count):
        buffer = pltpu.VMEM((count, kv_heads, page_size, head_dim), jnp.bfloat16)
        return [
            pltpu.SMEM((count + GROUP,), jnp.int32),
            buffer,
            buffer,
            pltpu.SemaphoreType.DMA((2, count)),
        ]

    def page_limit(count):
        pages = 2 * count * kv_heads * page_size * head_dim * 2
        return pltpu.CompilerParams(vmem_limit_bytes=pages + SMALL_VMEM)

    asked = n_dp * capacity
    places = 1 << (capacity - 1).bit_length()
    stride = -(-(capacity + 1) * q_heads // 8) * 8
    response = pl.pallas_call(
        functools.partial(remote_kernel, n_heads, sessions),
        out_shape=jax.ShapeDtypeStruct((n_dp, stride, head_dim), jnp.bfloat16),
        in_specs=[VMEM, HBM, HBM],
        out_specs=VMEM,
        scratch_shapes=[
            pltpu.VMEM((2, n_dp, 128), jnp.int32),
            pltpu.VMEM((n_dp * places, q_heads, head_dim), jnp.float32),
            pltpu.VMEM((n_dp, q_heads, head_dim), jnp.float32),
            pltpu.VMEM((asked + GROUP, q_heads, head_dim), jnp.bfloat16),
            pltpu.SMEM((n_dp * places,), jnp.int32),
            *page_scratch(asked),
        ],
        compiler_params=page_limit(asked),
        name="remote_pages",
        cost_estimate=pl.CostEstimate(flops=10**8, transcendentals=0, bytes_accessed=10**7),
    )(recv, keys, values)
    back = lax.all_to_all(response, "dp", split_axis=0, concat_axis=0, tiled=True)
    held = sessions * pages_max
    accumulator = jax.ShapeDtypeStruct((sessions, q_heads, head_dim), jnp.float32)
    num, den, spread, place = pl.pallas_call(
        functools.partial(local_kernel, n_heads),
        out_shape=(
            accumulator,
            accumulator,
            jax.ShapeDtypeStruct((sessions * q_heads, n_dp * stride), jnp.bfloat16),
            jax.ShapeDtypeStruct((n_dp, 128), jnp.int32),
        ),
        in_specs=[VMEM, HBM, HBM, HBM, HBM, HBM, HBM],
        out_specs=(VMEM,) * 4,
        scratch_shapes=[
            pltpu.SMEM((sessions, pages_max), jnp.int32),
            pltpu.SMEM(plan.shape, jnp.int32),
            pltpu.SMEM((1, sessions), jnp.int32),
            pltpu.VMEM(queries.shape, queries.dtype),
            pltpu.SemaphoreType.DMA((4,)),
            pltpu.SMEM((slot_total,), jnp.int32),
            pltpu.SMEM((slot_total,), jnp.int32),
            pltpu.SMEM((n_dp,), jnp.int32),
            *page_scratch(held),
        ],
        compiler_params=page_limit(held),
        name="local_pages",
        cost_estimate=pl.CostEstimate(flops=10**9, transcendentals=0, bytes_accessed=10**7),
    )(recv, table, plan, done, query, keys, values)
    return pl.pallas_call(
        functools.partial(combine_kernel, capacity),
        out_shape=jax.ShapeDtypeStruct((sessions, q_heads, head_dim), jnp.bfloat16),
        in_specs=[VMEM] * 5,
        out_specs=VMEM,
        compiler_params=pltpu.CompilerParams(vmem_limit_bytes=SMALL_VMEM),
        name="combine",
    )(back, num, den, spread, place)


def solution(mesh):
    in_specs = (
        P("dp", "heads", None),
        P("dp", "heads", None, None),
        P("dp", "heads", None, None),
        P("dp", "heads"),
        P("dp", None),
        P("dp"),
        P("dp", None),
    )
    out_specs = P("dp", "heads", None)
    return jax.shard_map(body, mesh=mesh, in_specs=in_specs, out_specs=out_specs, check_vma=False)
```

```python
import functools
import math

import jax
import jax.numpy as jnp
from jax import lax
from jax.experimental import pallas as pl
from jax.experimental.pallas import tpu as pltpu
from jax.sharding import PartitionSpec as P

softcap_limit = 50.0
score_divisor = 12.0
exp_scale = softcap_limit * math.log2(math.e)
GROUP = 5
LEN_BITS = 7
LEN_BASE = 1 << LEN_BITS
SMALL_VMEM = 4 << 20
SESS_LANE, PAGE_LANE, HIGH_LANE, LOW_LANE = 32, 64, 96, 112

VMEM = pl.BlockSpec(memory_space=pltpu.VMEM)
HBM = pl.BlockSpec(memory_space=pltpu.HBM)


def in_hbm(array):
    return pltpu.with_memory_space_constraint(array, pltpu.HBM)


def load_all(pairs, sems):
    copies = [pltpu.make_async_copy(s, d, sems.at[i]) for i, (s, d) in enumerate(pairs)]
    for copy in copies:
        copy.start()
    return copies


def pack_kernel(
    n_heads, len_hbm, table_hbm, plan_hbm, query_hbm, out_ref,
    len_ref, table_ref, plan_ref, query_ref, sems, owner, count, meta,
):
    copies = load_all(
        [(len_hbm, len_ref), (table_hbm, table_ref), (plan_hbm, plan_ref), (query_hbm, query_ref)],
        sems,
    )
    sessions, pages_max = table_ref.shape
    moves = plan_ref.shape[1]
    devices, tiles = out_ref.shape[:2]
    n_dp = devices // n_heads
    rows = out_ref.shape[2]
    parts = query_ref.shape[1] // rows
    head = lax.axis_index("heads")
    lane = lax.broadcasted_iota(jnp.int32, (1, 128), 1)
    base = jnp.zeros((1, 128), jnp.int32)
    for d in range(n_dp):
        count[d] = 0
    for copy in copies[:2]:
        copy.wait()
    for s in range(sessions):
        length = len_ref[0, s]
        base = jnp.where(lane == HIGH_LANE + s, length >> LEN_BITS, base)
        base = jnp.where(lane == LOW_LANE + s, length & (LEN_BASE - 1), base)
        for p in range(pages_max):
            owner[table_ref[s, p]] = s * 256 + p
    for d in range(n_dp):
        meta[d] = base
    for copy in copies[2:]:
        copy.wait()
    for r in range(moves):
        source = plan_ref[0, r]
        rank = count[source]
        count[source] = rank + 1
        entry = owner[plan_ref[2, r]]
        session = entry >> 8
        row = meta[source]
        row = jnp.where(lane == rank, plan_ref[1, r] + 1, row)
        row = jnp.where(lane == SESS_LANE + rank, session, row)
        row = jnp.where(lane == PAGE_LANE + rank, entry & 255, row)
        meta[source] = row
        tile = query_ref[session]
        for k in range(parts):
            out_ref[source * n_heads + head, rank * parts + k] = tile[k * rows : (k + 1) * rows]
    for d in range(n_dp):
        row = jnp.broadcast_to(meta[d].astype(jnp.float32), (rows, 128)).astype(jnp.bfloat16)
        for h in range(n_heads):
            out_ref[d * n_heads + h, tiles - 1] = row


def decode(recv_ref, index):
    tile = recv_ref[index, recv_ref.shape[1] - 1]
    return tile.astype(jnp.float32).astype(jnp.int32)[0:1]


def longest_of(recv_ref, d, n_heads):
    longest = None
    for h in range(n_heads):
        block = decode(recv_ref, d * n_heads + h)
        length = block * LEN_BASE + pltpu.roll(block, 128 - (LOW_LANE - HIGH_LANE), 1)
        longest = length if longest is None else jnp.maximum(longest, length)
    return longest


class Pages:
    def __init__(
        self, key_hbm, value_hbm, words, key_buf, value_buf, sems, num, den, per_device=None,
        lives=None,
    ):
        self.key_hbm, self.value_hbm, self.words = key_hbm, value_hbm, words
        self.key_buf, self.value_buf, self.sems = key_buf, value_buf, sems
        self.num, self.den, self.per_device, self.lives = num, den, per_device, lives
        self.kv_heads, self.page_size = key_hbm.shape[1:3]
        self.rows = num.shape[1]
        self.group = self.rows // self.kv_heads
        self.live_shift = key_hbm.shape[0].bit_length()
        self.row_shift = self.live_shift + self.page_size.bit_length()

    def word(self, slot, live, row):
        return (slot + 1) + live * (1 << self.live_shift) + row * (1 << self.row_shift)

    def slot(self, word):
        return (word & ((1 << self.live_shift) - 1)) - 1

    def live(self, i):
        if self.lives is not None:
            return jnp.where(self.words[i] > 0, self.lives[self.row(i)], 0)
        return (self.words[i] >> self.live_shift) & (2 * self.page_size - 1)

    def row(self, i):
        return self.words[i] >> self.row_shift

    def buffer(self, i):
        return jnp.minimum(i, self.total - 1)

    def start(self, i, slot, which):
        buf, hbm = (self.key_buf, self.key_hbm) if which == 0 else (self.value_buf, self.value_hbm)
        pltpu.make_async_copy(hbm.at[slot], buf.at[i], self.sems.at[which, i]).start()

    def add(self, total, needed, word):
        @pl.when(needed)
        def _():
            self.start(total, self.slot(word), 0)
            self.words[total] = word

        @pl.when(needed & (total >= GROUP))
        def _():
            before = total - GROUP
            self.start(before, self.slot(self.words[before]), 1)

        return total + needed.astype(jnp.int32)

    def wait(self, first, which):
        buf, hbm = (self.key_buf, self.key_hbm) if which == 0 else (self.value_buf, self.value_hbm)
        for j in range(GROUP):
            i = first + j

            @pl.when(i < self.total)
            def _(i=i):
                pltpu.make_async_copy(hbm.at[0], buf.at[i], self.sems.at[which, i]).wait()

    def scores(self, first, get_query):
        raws = []
        for j in range(GROUP):
            i = first + j
            query = get_query(i)
            buffer = self.buffer(i)
            raws.append(
                [
                    lax.dot_general(
                        query,
                        self.key_buf[buffer, k],
                        (((1,), (1,)), ((), ())),
                        preferred_element_type=jnp.float32,
                    )
                    for k in range(self.kv_heads)
                ]
            )
        return raws

    def select(self, parts):
        row = lax.broadcasted_iota(jnp.int32, parts[0].shape, 0)
        out = parts[-1]
        for k in reversed(range(self.kv_heads - 1)):
            out = jnp.where(row < (k + 1) * self.group, parts[k], out)
        return out

    def weights(self, first, raws):
        out = []
        place = lax.broadcasted_iota(jnp.int32, (self.rows, self.page_size), 1)
        for j in range(GROUP):
            raw = self.select(raws[j])
            capped = jnp.tanh(raw * (1.0 / (score_divisor * softcap_limit)))
            weight = jnp.exp2(capped * exp_scale)
            live = self.live(first + j)
            out.append(jnp.where(place < live, weight, 0.0).astype(jnp.bfloat16))
        return out

    def products(self, first, weights):
        parts = []
        for j in range(GROUP):
            buffer = self.buffer(first + j)
            parts.append(
                [
                    jnp.dot(
                        weights[j], self.value_buf[buffer, k], preferred_element_type=jnp.float32
                    )
                    for k in range(self.kv_heads)
                ]
            )
        return parts

    def accumulate(self, first, weights, parts):
        for j in range(GROUP):
            row = self.row(first + j)
            total = jnp.sum(weights[j].astype(jnp.float32), axis=1, keepdims=True)
            out = self.select(parts[j])
            self.num[row] = self.num[row] + out
            total = jnp.broadcast_to(total, out.shape)
            if self.per_device:
                lane = lax.broadcasted_iota(jnp.int32, out.shape, 1)
                total = jnp.where(lane == (row & (self.per_device - 1)), total, 0.0)
                row = row >> (self.per_device.bit_length() - 1)
            self.den[row] = self.den[row] + total

    def run(self, total, get_query):
        for j in range(GROUP):
            self.words[total + j] = 0

        @pl.when(total == 0)
        def _():
            self.start(0, 0, 0)
            self.words[0] = self.word(0, 0, 0)

        total = jnp.maximum(total, 1)
        self.total = total

        def rest(i, carry):
            self.start(i, self.slot(self.words[i]), 1)
            return carry

        lax.fori_loop(jnp.maximum(total - GROUP, 0), total, rest, 0)
        groups = (total + GROUP - 1) // GROUP
        self.wait(0, 0)
        weights = self.weights(0, self.scores(0, get_query))

        def step(g, weights):
            first = g * GROUP
            before = first - GROUP
            self.wait(first, 0)
            self.wait(before, 1)
            raws = self.scores(first, get_query)
            parts = self.products(before, weights)
            later = self.weights(first, raws)
            self.accumulate(before, weights, parts)
            return later

        weights = lax.fori_loop(1, groups, step, weights)
        last = (groups - 1) * GROUP
        self.wait(last, 1)
        self.accumulate(last, weights, self.products(last, weights))


def remote_kernel(
    n_heads, sessions, recv_ref, key_hbm, value_hbm, out_ref,
    meta, num, den, queries, lives, words, key_buf, value_buf, sems,
):
    devices, tiles, part_rows = recv_ref.shape[:3]
    rows = num.shape[1]
    n_dp = devices // n_heads
    parts = rows // part_rows
    capacity = (tiles - 1) // parts
    places = num.shape[0] // n_dp
    page_size = key_hbm.shape[2]
    head = lax.axis_index("heads")
    for d in range(n_dp):
        meta[0, d : d + 1, :] = decode(recv_ref, d * n_heads + head)
    own = meta[0]
    pages = Pages(
        key_hbm, value_hbm, words, key_buf, value_buf, sems, num, den, places, lives
    )
    total = jnp.int32(0)
    for d in range(n_dp):
        for c in range(capacity):
            slot = own[d, c]
            for k in range(parts):
                queries[total, k * part_rows : (k + 1) * part_rows] = recv_ref[
                    d * n_heads + head, c * parts + k
                ]
            total = pages.add(total, slot > 0, pages.word(slot - 1, 0, d * places + c))

    for d in range(n_dp):
        meta[1, d : d + 1, :] = longest_of(recv_ref, d, n_heads)
    longest = meta[1]
    session = pltpu.roll(own, 128 - SESS_LANE, 1)
    page = pltpu.roll(own, 128 - PAGE_LANE, 1)
    length = jnp.zeros_like(own)
    for s in range(sessions):
        known = jnp.broadcast_to(longest[:, HIGH_LANE + s : HIGH_LANE + s + 1], own.shape)
        length = jnp.where(session == s, known, length)
    live = jnp.where(own > 0, jnp.clip(length - page * page_size, 0, page_size), 0)
    for d in range(n_dp):
        for c in range(capacity):
            lives[d * places + c] = live[d, c]
    num[...] = jnp.zeros_like(num)
    den[...] = jnp.zeros_like(den)
    pages.run(total, lambda i: queries[i])

    for d in range(n_dp):
        for c in range(capacity):
            out_ref[d, c * rows : (c + 1) * rows] = num[d * places + c].astype(jnp.bfloat16)
        high = den[d].astype(jnp.bfloat16).astype(jnp.float32)
        used = (capacity + 1) * rows
        out_ref[d, used - rows : used] = (high + pltpu.roll(den[d] - high, 64, 1)).astype(
            jnp.bfloat16
        )
        if used < out_ref.shape[1]:
            out_ref[d, used:] = jnp.zeros((out_ref.shape[1] - used, 128), jnp.bfloat16)


def local_kernel(
    n_heads, recv_ref, table_hbm, plan_hbm, finished_hbm, query_hbm, key_hbm, value_hbm,
    num, den, spread_ref, place_ref, table_ref, plan_ref, finished_ref, query_ref, loads,
    moved, owner, count, words, key_buf, value_buf, sems,
):
    copies = load_all(
        [
            (table_hbm, table_ref),
            (plan_hbm, plan_ref),
            (finished_hbm, finished_ref),
            (query_hbm, query_ref),
        ],
        loads,
    )
    sessions, pages_max = table_ref.shape
    page_size = key_hbm.shape[2]
    slots = key_hbm.shape[0]
    longest = longest_of(recv_ref, lax.axis_index("dp"), n_heads)
    num[...] = jnp.zeros_like(num)
    for j in range(slots):
        moved[j] = 0
    for load in copies:
        load.wait()
    for s in range(sessions):
        den[s] = jnp.full(den.shape[1:], 1.0, jnp.float32) * finished_ref[0, s].astype(jnp.float32)
    for r in range(plan_ref.shape[1]):
        moved[plan_ref[2, r]] = 1
    pages = Pages(key_hbm, value_hbm, words, key_buf, value_buf, sems, num, den)
    total = jnp.int32(0)
    for s in range(sessions):
        length = jnp.where(finished_ref[0, s] == 1, 0, longest[0, HIGH_LANE + s])
        for p in range(pages_max):
            slot = table_ref[s, p]
            live = jnp.clip(length - p * page_size, 0, page_size)
            needed = (live > 0) & (moved[slot] == 0)
            total = pages.add(total, needed, pages.word(slot, live, s))
    pages.run(total, lambda i: query_ref[pages.row(i)])

    n_dp = place_ref.shape[0]
    rows = num.shape[1]
    stride = spread_ref.shape[1] // n_dp
    for s in range(sessions):
        for p in range(pages_max):
            owner[table_ref[s, p]] = s
    for d in range(n_dp):
        count[d] = 0
    row = lax.broadcasted_iota(jnp.int32, spread_ref.shape, 0)
    column = lax.broadcasted_iota(jnp.int32, spread_ref.shape, 1)
    device = lax.broadcasted_iota(jnp.int32, place_ref.shape, 0)
    lane = lax.broadcasted_iota(jnp.int32, place_ref.shape, 1) & 63
    session_row = row // rows
    spread = jnp.zeros(spread_ref.shape, jnp.float32)
    places = jnp.full(place_ref.shape, -1, jnp.int32)
    for r in range(plan_ref.shape[1]):
        source = plan_ref[0, r]
        rank = count[source]
        count[source] = rank + 1
        session = owner[plan_ref[2, r]]
        offset = source * stride + rank * rows - session * rows
        spread = jnp.where((column - row == offset) & (session_row == session), 1.0, spread)
        places = jnp.where((device == source) & (lane == rank), session, places)
    spread_ref[...] = spread.astype(jnp.bfloat16)
    place_ref[...] = places


def combine_kernel(capacity, back_ref, num_ref, den_ref, spread_ref, place_ref, out_ref):
    n_dp, stride = back_ref.shape[:2]
    sessions, rows = num_ref.shape[:2]
    moved = jnp.dot(
        spread_ref[...],
        back_ref[...].reshape(n_dp * stride, 128),
        preferred_element_type=jnp.float32,
    )
    tile = slice(capacity * rows, (capacity + 1) * rows)
    weights = [back_ref[d, tile].astype(jnp.float32) for d in range(n_dp)]
    for s in range(sessions):
        packed = jnp.zeros((rows, 128), jnp.float32)
        for d in range(n_dp):
            mine = jnp.broadcast_to(place_ref[d : d + 1, :], (rows, 128)) == s
            packed = packed + jnp.where(mine, weights[d], 0.0)
        weight = den_ref[s] + jnp.sum(packed, axis=1, keepdims=True)
        total = num_ref[s] + moved[s * rows : (s + 1) * rows]
        out_ref[s] = (total / weight).astype(jnp.bfloat16)


def body(queries, key_cache, value_cache, lengths_seen, page_table, finished, move_plan):
    slot_total, kv_heads, page_size, head_dim = key_cache.shape
    sessions, q_heads, _ = queries.shape
    pages_max = page_table.shape[1]
    moves = move_plan.shape[0]
    n_dp = lax.axis_size("dp")
    n_heads = lax.axis_size("heads")
    capacity = (moves - 1) // (n_dp - 1) + 1
    assert capacity <= 32 and sessions <= 16 and slot_total < 256 and pages_max <= 256
    assert page_size & (page_size - 1) == 0 and sessions & (sessions - 1) == 0
    assert n_dp * sessions << 8 << 10 < 2**31

    seen = in_hbm(lengths_seen.T)
    plan = in_hbm(move_plan.T)
    table = in_hbm(page_table)
    query = in_hbm(queries)
    done = in_hbm(finished.reshape(1, sessions))
    keys = in_hbm(key_cache)
    values = in_hbm(value_cache)

    packed = pl.pallas_call(
        functools.partial(pack_kernel, n_heads),
        out_shape=jax.ShapeDtypeStruct(
            (n_dp * n_heads, capacity * kv_heads + 1, q_heads // kv_heads, head_dim), jnp.bfloat16
        ),
        in_specs=[HBM] * 4,
        out_specs=VMEM,
        scratch_shapes=[
            pltpu.SMEM((1, sessions), jnp.int32),
            pltpu.SMEM((sessions, pages_max), jnp.int32),
            pltpu.SMEM(plan.shape, jnp.int32),
            pltpu.VMEM(queries.shape, queries.dtype),
            pltpu.SemaphoreType.DMA((4,)),
            pltpu.SMEM((slot_total,), jnp.int32),
            pltpu.SMEM((n_dp,), jnp.int32),
            pltpu.VMEM((n_dp, 1, 128), jnp.int32),
        ],
        compiler_params=pltpu.CompilerParams(vmem_limit_bytes=SMALL_VMEM),
        name="pack",
    )(seen, table, plan, query)
    recv = lax.all_to_all(packed, ("dp", "heads"), split_axis=0, concat_axis=0, tiled=True)

    def page_scratch(count):
        buffer = pltpu.VMEM((count, kv_heads, page_size, head_dim), jnp.bfloat16)
        return [
            pltpu.SMEM((count + GROUP,), jnp.int32),
            buffer,
            buffer,
            pltpu.SemaphoreType.DMA((2, count)),
        ]

    def page_limit(count):
        pages = 2 * count * kv_heads * page_size * head_dim * 2
        return pltpu.CompilerParams(vmem_limit_bytes=pages + SMALL_VMEM)

    asked = n_dp * capacity
    places = 1 << (capacity - 1).bit_length()
    stride = -(-(capacity + 1) * q_heads // 8) * 8
    response = pl.pallas_call(
        functools.partial(remote_kernel, n_heads, sessions),
        out_shape=jax.ShapeDtypeStruct((n_dp, stride, head_dim), jnp.bfloat16),
        in_specs=[VMEM, HBM, HBM],
        out_specs=VMEM,
        scratch_shapes=[
            pltpu.VMEM((2, n_dp, 128), jnp.int32),
            pltpu.VMEM((n_dp * places, q_heads, head_dim), jnp.float32),
            pltpu.VMEM((n_dp, q_heads, head_dim), jnp.float32),
            pltpu.VMEM((asked + GROUP, q_heads, head_dim), jnp.bfloat16),
            pltpu.SMEM((n_dp * places,), jnp.int32),
            *page_scratch(asked),
        ],
        compiler_params=page_limit(asked),
        name="remote_pages",
        cost_estimate=pl.CostEstimate(flops=10**8, transcendentals=0, bytes_accessed=10**7),
    )(recv, keys, values)
    back = lax.all_to_all(response, "dp", split_axis=0, concat_axis=0, tiled=True)
    held = sessions * pages_max
    accumulator = jax.ShapeDtypeStruct((sessions, q_heads, head_dim), jnp.float32)
    num, den, spread, place = pl.pallas_call(
        functools.partial(local_kernel, n_heads),
        out_shape=(
            accumulator,
            accumulator,
            jax.ShapeDtypeStruct((sessions * q_heads, n_dp * stride), jnp.bfloat16),
            jax.ShapeDtypeStruct((n_dp, 128), jnp.int32),
        ),
        in_specs=[VMEM, HBM, HBM, HBM, HBM, HBM, HBM],
        out_specs=(VMEM,) * 4,
        scratch_shapes=[
            pltpu.SMEM((sessions, pages_max), jnp.int32),
            pltpu.SMEM(plan.shape, jnp.int32),
            pltpu.SMEM((1, sessions), jnp.int32),
            pltpu.VMEM(queries.shape, queries.dtype),
            pltpu.SemaphoreType.DMA((4,)),
            pltpu.SMEM((slot_total,), jnp.int32),
            pltpu.SMEM((slot_total,), jnp.int32),
            pltpu.SMEM((n_dp,), jnp.int32),
            *page_scratch(held),
        ],
        compiler_params=page_limit(held),
        name="local_pages",
        cost_estimate=pl.CostEstimate(flops=10**9, transcendentals=0, bytes_accessed=10**7),
    )(recv, table, plan, done, query, keys, values)
    return pl.pallas_call(
        functools.partial(combine_kernel, capacity),
        out_shape=jax.ShapeDtypeStruct((sessions, q_heads, head_dim), jnp.bfloat16),
        in_specs=[VMEM] * 5,
        out_specs=VMEM,
        compiler_params=pltpu.CompilerParams(vmem_limit_bytes=SMALL_VMEM),
        name="combine",
    )(back, num, den, spread, place)


def solution(mesh):
    in_specs = (
        P("dp", "heads", None),
        P("dp", "heads", None, None),
        P("dp", "heads", None, None),
        P("dp", "heads"),
        P("dp", None),
        P("dp"),
        P("dp", None),
    )
    out_specs = P("dp", "heads", None)
    return jax.shard_map(body, mesh=mesh, in_specs=in_specs, out_specs=out_specs, check_vma=False)
```

```python
import functools
import math

import jax
import jax.numpy as jnp
from jax import lax
from jax.experimental import pallas as pl
from jax.experimental.pallas import tpu as pltpu
from jax.sharding import PartitionSpec as P

softcap_limit = 50.0
score_divisor = 12.0
exp_scale = softcap_limit * math.log2(math.e)
GROUP = 7
LEN_BITS = 7
LEN_BASE = 1 << LEN_BITS
SMALL_VMEM = 4 << 20
SESS_LANE, PAGE_LANE, HIGH_LANE, LOW_LANE = 32, 64, 96, 112

VMEM = pl.BlockSpec(memory_space=pltpu.VMEM)
HBM = pl.BlockSpec(memory_space=pltpu.HBM)


def in_hbm(array):
    return pltpu.with_memory_space_constraint(array, pltpu.HBM)


def load_all(pairs, sems):
    copies = [pltpu.make_async_copy(s, d, sems.at[i]) for i, (s, d) in enumerate(pairs)]
    for copy in copies:
        copy.start()
    return copies


def pack_kernel(
    n_heads, len_hbm, table_hbm, plan_hbm, query_hbm, out_ref,
    len_ref, table_ref, plan_ref, query_ref, sems, owner, count, meta,
):
    copies = load_all(
        [(len_hbm, len_ref), (table_hbm, table_ref), (plan_hbm, plan_ref), (query_hbm, query_ref)],
        sems,
    )
    sessions, pages_max = table_ref.shape
    moves = plan_ref.shape[1]
    devices, tiles = out_ref.shape[:2]
    n_dp = devices // n_heads
    rows = out_ref.shape[2]
    parts = query_ref.shape[1] // rows
    head = lax.axis_index("heads")
    lane = lax.broadcasted_iota(jnp.int32, (1, 128), 1)
    base = jnp.zeros((1, 128), jnp.int32)
    for d in range(n_dp):
        count[d] = 0
    for copy in copies[:2]:
        copy.wait()
    for s in range(sessions):
        length = len_ref[0, s]
        base = jnp.where(lane == HIGH_LANE + s, length >> LEN_BITS, base)
        base = jnp.where(lane == LOW_LANE + s, length & (LEN_BASE - 1), base)
        for p in range(pages_max):
            owner[table_ref[s, p]] = s * 256 + p
    for d in range(n_dp):
        meta[d] = base
    for copy in copies[2:]:
        copy.wait()
    for r in range(moves):
        source = plan_ref[0, r]
        rank = count[source]
        count[source] = rank + 1
        entry = owner[plan_ref[2, r]]
        session = entry >> 8
        row = meta[source]
        row = jnp.where(lane == rank, plan_ref[1, r] + 1, row)
        row = jnp.where(lane == SESS_LANE + rank, session, row)
        row = jnp.where(lane == PAGE_LANE + rank, entry & 255, row)
        meta[source] = row
        tile = query_ref[session]
        for k in range(parts):
            out_ref[source * n_heads + head, rank * parts + k] = tile[k * rows : (k + 1) * rows]
    for d in range(n_dp):
        row = jnp.broadcast_to(meta[d].astype(jnp.float32), (rows, 128)).astype(jnp.bfloat16)
        for h in range(n_heads):
            out_ref[d * n_heads + h, tiles - 1] = row


def decode(recv_ref, index):
    tile = recv_ref[index, recv_ref.shape[1] - 1]
    return tile.astype(jnp.float32).astype(jnp.int32)[0:1]


def longest_of(recv_ref, d, n_heads):
    longest = None
    for h in range(n_heads):
        block = decode(recv_ref, d * n_heads + h)
        length = block * LEN_BASE + pltpu.roll(block, 128 - (LOW_LANE - HIGH_LANE), 1)
        longest = length if longest is None else jnp.maximum(longest, length)
    return longest


class Pages:
    def __init__(
        self, key_hbm, value_hbm, words, key_buf, value_buf, sems, num, den, per_device=None,
        lives=None,
    ):
        self.key_hbm, self.value_hbm, self.words = key_hbm, value_hbm, words
        self.key_buf, self.value_buf, self.sems = key_buf, value_buf, sems
        self.num, self.den, self.per_device, self.lives = num, den, per_device, lives
        self.kv_heads, self.page_size = key_hbm.shape[1:3]
        self.rows = num.shape[1]
        self.group = self.rows // self.kv_heads
        self.live_shift = key_hbm.shape[0].bit_length()
        self.row_shift = self.live_shift + self.page_size.bit_length()

    def word(self, slot, live, row):
        return (slot + 1) + live * (1 << self.live_shift) + row * (1 << self.row_shift)

    def slot(self, word):
        return (word & ((1 << self.live_shift) - 1)) - 1

    def live(self, i):
        if self.lives is not None:
            return jnp.where(self.words[i] > 0, self.lives[self.row(i)], 0)
        return (self.words[i] >> self.live_shift) & (2 * self.page_size - 1)

    def row(self, i):
        return self.words[i] >> self.row_shift

    def buffer(self, i):
        return jnp.minimum(i, self.total - 1)

    def start(self, i, slot, which):
        buf, hbm = (self.key_buf, self.key_hbm) if which == 0 else (self.value_buf, self.value_hbm)
        pltpu.make_async_copy(hbm.at[slot], buf.at[i], self.sems.at[which, i]).start()

    def add(self, total, needed, word):
        @pl.when(needed)
        def _():
            self.start(total, self.slot(word), 0)
            self.words[total] = word

        @pl.when(needed & (total >= GROUP))
        def _():
            before = total - GROUP
            self.start(before, self.slot(self.words[before]), 1)

        return total + needed.astype(jnp.int32)

    def wait(self, first, which):
        buf, hbm = (self.key_buf, self.key_hbm) if which == 0 else (self.value_buf, self.value_hbm)
        for j in range(GROUP):
            i = first + j

            @pl.when(i < self.total)
            def _(i=i):
                pltpu.make_async_copy(hbm.at[0], buf.at[i], self.sems.at[which, i]).wait()

    def scores(self, first, get_query):
        raws = []
        for j in range(GROUP):
            i = first + j
            query = get_query(i)
            buffer = self.buffer(i)
            raws.append(
                [
                    lax.dot_general(
                        query,
                        self.key_buf[buffer, k],
                        (((1,), (1,)), ((), ())),
                        preferred_element_type=jnp.float32,
                    )
                    for k in range(self.kv_heads)
                ]
            )
        return raws

    def select(self, parts):
        row = lax.broadcasted_iota(jnp.int32, parts[0].shape, 0)
        out = parts[-1]
        for k in reversed(range(self.kv_heads - 1)):
            out = jnp.where(row < (k + 1) * self.group, parts[k], out)
        return out

    def weights(self, first, raws):
        out = []
        place = lax.broadcasted_iota(jnp.int32, (self.rows, self.page_size), 1)
        for j in range(GROUP):
            raw = self.select(raws[j])
            capped = jnp.tanh(raw * (1.0 / (score_divisor * softcap_limit)))
            weight = jnp.exp2(capped * exp_scale)
            live = self.live(first + j)
            out.append(jnp.where(place < live, weight, 0.0).astype(jnp.bfloat16))
        return out

    def products(self, first, weights):
        parts = []
        for j in range(GROUP):
            buffer = self.buffer(first + j)
            parts.append(
                [
                    jnp.dot(
                        weights[j], self.value_buf[buffer, k], preferred_element_type=jnp.float32
                    )
                    for k in range(self.kv_heads)
                ]
            )
        return parts

    def accumulate(self, first, weights, parts):
        for j in range(GROUP):
            row = self.row(first + j)
            total = jnp.sum(weights[j].astype(jnp.float32), axis=1, keepdims=True)
            out = self.select(parts[j])
            self.num[row] = self.num[row] + out
            total = jnp.broadcast_to(total, out.shape)
            if self.per_device:
                lane = lax.broadcasted_iota(jnp.int32, out.shape, 1)
                total = jnp.where(lane == (row & (self.per_device - 1)), total, 0.0)
                row = row >> (self.per_device.bit_length() - 1)
            self.den[row] = self.den[row] + total

    def run(self, total, get_query):
        for j in range(GROUP):
            self.words[total + j] = 0

        @pl.when(total == 0)
        def _():
            self.start(0, 0, 0)
            self.words[0] = self.word(0, 0, 0)

        total = jnp.maximum(total, 1)
        self.total = total

        def rest(i, carry):
            self.start(i, self.slot(self.words[i]), 1)
            return carry

        lax.fori_loop(jnp.maximum(total - GROUP, 0), total, rest, 0)
        groups = (total + GROUP - 1) // GROUP
        self.wait(0, 0)
        weights = self.weights(0, self.scores(0, get_query))

        def step(g, weights):
            first = g * GROUP
            before = first - GROUP
            self.wait(first, 0)
            self.wait(before, 1)
            raws = self.scores(first, get_query)
            parts = self.products(before, weights)
            later = self.weights(first, raws)
            self.accumulate(before, weights, parts)
            return later

        weights = lax.fori_loop(1, groups, step, weights)
        last = (groups - 1) * GROUP
        self.wait(last, 1)
        self.accumulate(last, weights, self.products(last, weights))


def remote_kernel(
    n_heads, sessions, recv_ref, key_hbm, value_hbm, out_ref,
    meta, num, den, queries, lives, words, key_buf, value_buf, sems,
):
    devices, tiles, part_rows = recv_ref.shape[:3]
    rows = num.shape[1]
    n_dp = devices // n_heads
    parts = rows // part_rows
    capacity = (tiles - 1) // parts
    places = num.shape[0] // n_dp
    page_size = key_hbm.shape[2]
    head = lax.axis_index("heads")
    for d in range(n_dp):
        meta[0, d : d + 1, :] = decode(recv_ref, d * n_heads + head)
    own = meta[0]
    pages = Pages(
        key_hbm, value_hbm, words, key_buf, value_buf, sems, num, den, places, lives
    )
    total = jnp.int32(0)
    for d in range(n_dp):
        for c in range(capacity):
            slot = own[d, c]
            for k in range(parts):
                queries[total, k * part_rows : (k + 1) * part_rows] = recv_ref[
                    d * n_heads + head, c * parts + k
                ]
            total = pages.add(total, slot > 0, pages.word(slot - 1, 0, d * places + c))

    for d in range(n_dp):
        meta[1, d : d + 1, :] = longest_of(recv_ref, d, n_heads)
    longest = meta[1]
    session = pltpu.roll(own, 128 - SESS_LANE, 1)
    page = pltpu.roll(own, 128 - PAGE_LANE, 1)
    length = jnp.zeros_like(own)
    for s in range(sessions):
        known = jnp.broadcast_to(longest[:, HIGH_LANE + s : HIGH_LANE + s + 1], own.shape)
        length = jnp.where(session == s, known, length)
    live = jnp.where(own > 0, jnp.clip(length - page * page_size, 0, page_size), 0)
    for d in range(n_dp):
        for c in range(capacity):
            lives[d * places + c] = live[d, c]
    num[...] = jnp.zeros_like(num)
    den[...] = jnp.zeros_like(den)
    pages.run(total, lambda i: queries[i])

    for d in range(n_dp):
        for c in range(capacity):
            out_ref[d, c * rows : (c + 1) * rows] = num[d * places + c].astype(jnp.bfloat16)
        high = den[d].astype(jnp.bfloat16).astype(jnp.float32)
        used = (capacity + 1) * rows
        out_ref[d, used - rows : used] = (high + pltpu.roll(den[d] - high, 64, 1)).astype(
            jnp.bfloat16
        )
        if used < out_ref.shape[1]:
            out_ref[d, used:] = jnp.zeros((out_ref.shape[1] - used, 128), jnp.bfloat16)


def local_kernel(
    n_heads, recv_ref, table_hbm, plan_hbm, finished_hbm, query_hbm, key_hbm, value_hbm,
    num, den, spread_ref, place_ref, table_ref, plan_ref, finished_ref, query_ref, loads,
    moved, owner, count, words, key_buf, value_buf, sems,
):
    copies = load_all(
        [
            (table_hbm, table_ref),
            (plan_hbm, plan_ref),
            (finished_hbm, finished_ref),
            (query_hbm, query_ref),
        ],
        loads,
    )
    sessions, pages_max = table_ref.shape
    page_size = key_hbm.shape[2]
    slots = key_hbm.shape[0]
    longest = longest_of(recv_ref, lax.axis_index("dp"), n_heads)
    num[...] = jnp.zeros_like(num)
    for j in range(slots):
        moved[j] = 0
    for load in copies:
        load.wait()
    for s in range(sessions):
        den[s] = jnp.full(den.shape[1:], 1.0, jnp.float32) * finished_ref[0, s].astype(jnp.float32)
    for r in range(plan_ref.shape[1]):
        moved[plan_ref[2, r]] = 1
    pages = Pages(key_hbm, value_hbm, words, key_buf, value_buf, sems, num, den)
    total = jnp.int32(0)
    for s in range(sessions):
        length = jnp.where(finished_ref[0, s] == 1, 0, longest[0, HIGH_LANE + s])
        for p in range(pages_max):
            slot = table_ref[s, p]
            live = jnp.clip(length - p * page_size, 0, page_size)
            needed = (live > 0) & (moved[slot] == 0)
            total = pages.add(total, needed, pages.word(slot, live, s))
    pages.run(total, lambda i: query_ref[pages.row(i)])

    n_dp = place_ref.shape[0]
    rows = num.shape[1]
    stride = spread_ref.shape[1] // n_dp
    for s in range(sessions):
        for p in range(pages_max):
            owner[table_ref[s, p]] = s
    for d in range(n_dp):
        count[d] = 0
    row = lax.broadcasted_iota(jnp.int32, spread_ref.shape, 0)
    column = lax.broadcasted_iota(jnp.int32, spread_ref.shape, 1)
    device = lax.broadcasted_iota(jnp.int32, place_ref.shape, 0)
    lane = lax.broadcasted_iota(jnp.int32, place_ref.shape, 1) & 63
    session_row = row // rows
    spread = jnp.zeros(spread_ref.shape, jnp.float32)
    places = jnp.full(place_ref.shape, -1, jnp.int32)
    for r in range(plan_ref.shape[1]):
        source = plan_ref[0, r]
        rank = count[source]
        count[source] = rank + 1
        session = owner[plan_ref[2, r]]
        offset = source * stride + rank * rows - session * rows
        spread = jnp.where((column - row == offset) & (session_row == session), 1.0, spread)
        places = jnp.where((device == source) & (lane == rank), session, places)
    spread_ref[...] = spread.astype(jnp.bfloat16)
    place_ref[...] = places


def combine_kernel(capacity, back_ref, num_ref, den_ref, spread_ref, place_ref, out_ref):
    n_dp, stride = back_ref.shape[:2]
    sessions, rows = num_ref.shape[:2]
    moved = jnp.dot(
        spread_ref[...],
        back_ref[...].reshape(n_dp * stride, 128),
        preferred_element_type=jnp.float32,
    )
    tile = slice(capacity * rows, (capacity + 1) * rows)
    weights = [back_ref[d, tile].astype(jnp.float32) for d in range(n_dp)]
    for s in range(sessions):
        packed = jnp.zeros((rows, 128), jnp.float32)
        for d in range(n_dp):
            mine = jnp.broadcast_to(place_ref[d : d + 1, :], (rows, 128)) == s
            packed = packed + jnp.where(mine, weights[d], 0.0)
        weight = den_ref[s] + jnp.sum(packed, axis=1, keepdims=True)
        total = num_ref[s] + moved[s * rows : (s + 1) * rows]
        out_ref[s] = (total / weight).astype(jnp.bfloat16)


def body(queries, key_cache, value_cache, lengths_seen, page_table, finished, move_plan):
    slot_total, kv_heads, page_size, head_dim = key_cache.shape
    sessions, q_heads, _ = queries.shape
    pages_max = page_table.shape[1]
    moves = move_plan.shape[0]
    n_dp = lax.axis_size("dp")
    n_heads = lax.axis_size("heads")
    capacity = (moves - 1) // (n_dp - 1) + 1
    assert capacity <= 32 and sessions <= 16 and slot_total < 256 and pages_max <= 256
    assert page_size & (page_size - 1) == 0 and sessions & (sessions - 1) == 0
    assert n_dp * sessions << 8 << 10 < 2**31

    seen = in_hbm(lengths_seen.T)
    plan = in_hbm(move_plan.T)
    table = in_hbm(page_table)
    query = in_hbm(queries)
    done = in_hbm(finished.reshape(1, sessions))
    keys = in_hbm(key_cache)
    values = in_hbm(value_cache)

    packed = pl.pallas_call(
        functools.partial(pack_kernel, n_heads),
        out_shape=jax.ShapeDtypeStruct(
            (n_dp * n_heads, capacity * kv_heads + 1, q_heads // kv_heads, head_dim), jnp.bfloat16
        ),
        in_specs=[HBM] * 4,
        out_specs=VMEM,
        scratch_shapes=[
            pltpu.SMEM((1, sessions), jnp.int32),
            pltpu.SMEM((sessions, pages_max), jnp.int32),
            pltpu.SMEM(plan.shape, jnp.int32),
            pltpu.VMEM(queries.shape, queries.dtype),
            pltpu.SemaphoreType.DMA((4,)),
            pltpu.SMEM((slot_total,), jnp.int32),
            pltpu.SMEM((n_dp,), jnp.int32),
            pltpu.VMEM((n_dp, 1, 128), jnp.int32),
        ],
        compiler_params=pltpu.CompilerParams(vmem_limit_bytes=SMALL_VMEM),
        name="pack",
    )(seen, table, plan, query)
    recv = lax.all_to_all(packed, ("dp", "heads"), split_axis=0, concat_axis=0, tiled=True)

    def page_scratch(count):
        buffer = pltpu.VMEM((count, kv_heads, page_size, head_dim), jnp.bfloat16)
        return [
            pltpu.SMEM((count + GROUP,), jnp.int32),
            buffer,
            buffer,
            pltpu.SemaphoreType.DMA((2, count)),
        ]

    def page_limit(count):
        pages = 2 * count * kv_heads * page_size * head_dim * 2
        return pltpu.CompilerParams(vmem_limit_bytes=pages + SMALL_VMEM)

    asked = n_dp * capacity
    places = 1 << (capacity - 1).bit_length()
    stride = -(-(capacity + 1) * q_heads // 8) * 8
    response = pl.pallas_call(
        functools.partial(remote_kernel, n_heads, sessions),
        out_shape=jax.ShapeDtypeStruct((n_dp, stride, head_dim), jnp.bfloat16),
        in_specs=[VMEM, HBM, HBM],
        out_specs=VMEM,
        scratch_shapes=[
            pltpu.VMEM((2, n_dp, 128), jnp.int32),
            pltpu.VMEM((n_dp * places, q_heads, head_dim), jnp.float32),
            pltpu.VMEM((n_dp, q_heads, head_dim), jnp.float32),
            pltpu.VMEM((asked + GROUP, q_heads, head_dim), jnp.bfloat16),
            pltpu.SMEM((n_dp * places,), jnp.int32),
            *page_scratch(asked),
        ],
        compiler_params=page_limit(asked),
        name="remote_pages",
        cost_estimate=pl.CostEstimate(flops=10**8, transcendentals=0, bytes_accessed=10**7),
    )(recv, keys, values)
    back = lax.all_to_all(response, "dp", split_axis=0, concat_axis=0, tiled=True)
    held = sessions * pages_max
    accumulator = jax.ShapeDtypeStruct((sessions, q_heads, head_dim), jnp.float32)
    num, den, spread, place = pl.pallas_call(
        functools.partial(local_kernel, n_heads),
        out_shape=(
            accumulator,
            accumulator,
            jax.ShapeDtypeStruct((sessions * q_heads, n_dp * stride), jnp.bfloat16),
            jax.ShapeDtypeStruct((n_dp, 128), jnp.int32),
        ),
        in_specs=[VMEM, HBM, HBM, HBM, HBM, HBM, HBM],
        out_specs=(VMEM,) * 4,
        scratch_shapes=[
            pltpu.SMEM((sessions, pages_max), jnp.int32),
            pltpu.SMEM(plan.shape, jnp.int32),
            pltpu.SMEM((1, sessions), jnp.int32),
            pltpu.VMEM(queries.shape, queries.dtype),
            pltpu.SemaphoreType.DMA((4,)),
            pltpu.SMEM((slot_total,), jnp.int32),
            pltpu.SMEM((slot_total,), jnp.int32),
            pltpu.SMEM((n_dp,), jnp.int32),
            *page_scratch(held),
        ],
        compiler_params=page_limit(held),
        name="local_pages",
        cost_estimate=pl.CostEstimate(flops=10**9, transcendentals=0, bytes_accessed=10**7),
    )(recv, table, plan, done, query, keys, values)
    return pl.pallas_call(
        functools.partial(combine_kernel, capacity),
        out_shape=jax.ShapeDtypeStruct((sessions, q_heads, head_dim), jnp.bfloat16),
        in_specs=[VMEM] * 5,
        out_specs=VMEM,
        compiler_params=pltpu.CompilerParams(vmem_limit_bytes=SMALL_VMEM),
        name="combine",
    )(back, num, den, spread, place)


def solution(mesh):
    in_specs = (
        P("dp", "heads", None),
        P("dp", "heads", None, None),
        P("dp", "heads", None, None),
        P("dp", "heads"),
        P("dp", None),
        P("dp"),
        P("dp", None),
    )
    out_specs = P("dp", "heads", None)
    return jax.shard_map(body, mesh=mesh, in_specs=in_specs, out_specs=out_specs, check_vma=False)
```
